32 devices in a mesh: expert: 4 (over z), vocab: 2 (over x), batch: 4 (over y, core).
Axes of the slice: x: 2, y: 2, z: 4, core: 2. Of those that a mesh axis runs over, the one named last changes fastest.
Arguments:
- resid: bfloat16 [4, 64, 6144], P('batch', ('expert', 'vocab')), may hold values from -6 to 6
- moe_gain: float32 [6144], replicated, may hold values from 0.25 to 2.5
- final_gain: float32 [6144], replicated, may hold values from 0.5 to 1.5
- router: bfloat16 [6144, 4], replicated, may hold values from -0.078125 to 0.078125
- w_gate: bfloat16 [4, 6144, 8192], P('expert', None, ('vocab', 'batch')), may hold values from -0.078125 to 0.078125
- w_up: bfloat16 [4, 6144, 8192], P('expert', None, ('vocab', 'batch')), may hold values from -0.078125 to 0.078125
- w_down: bfloat16 [4, 8192, 6144], P('expert', ('vocab', 'batch')), may hold values from -0.0625 to 0.0625
- lm_head: bfloat16 [16384, 6144], P(('expert', 'vocab')), may hold values from -6 to 6
- expert_ids: int32 [4, 64, 2], P('batch', ('expert', 'vocab')), may hold values from 0 to 3, all different within a row; in each aligned block of 8 rows (0 to 7, 8 to 15, ..., all dimensions but the last counted through in order) at most 5 rows name the same one
- target_ids: int32 [4, 64], P('batch'), may hold values from 0 to 16383
- choice_len: int32 [4, 8], P('batch'), may hold values from 1 to 32, 64 in all within a row
- choice_question: int32 [4, 8], P('batch'), may hold values from 0 to 1, as said below
Outputs:
- token_logprob: float32 [4, 64], P('batch', ('expert', 'vocab'))
- choice_prob: float32 [4, 8], P('batch')
The draws below stay inside these ranges and needn't reach their ends.
Inputs may be any that keep to these rules, and one draw needn't show every extreme that they name: `expert_ids`: A token's 2 experts differ; the rows of one device name each expert at most 5 times. `choice_len`: each group's lengths sum to 64. `choice_question`: in each group every question number appears exactly four times.
All inputs are finite; a program needn't handle non-finite values.
Results may differ from the reference program's by a relative error of at most 0.019.
Values may be sent and summed in bfloat16 or wider, within the bound.
A program may use at most 128 MiB of HBM per device.

```python
import math
import jax
import jax.numpy as jnp
import numpy as np
from jax import lax

D = 6144
TOPK = 2
FF_WIN = 8192
VOC_WIN = 16384
TOK_DEV = 8
EXPERTS = 4
GROUP_TOK = 64
CHOICES = 8
MOSTLEN = 32
CAP = 5
N_EXPERT = 4
N_VOCAB = 2
N_BATCH = 4


def draw_resid(key, part):
    base_key = jax.random.fold_in(key, 707)
    values = jnp.clip(jax.random.normal(base_key, (N_BATCH * GROUP_TOK, D), jnp.float32), -6.0, 6.0)
    return values.reshape(N_BATCH, GROUP_TOK, D).astype(jnp.bfloat16)


def draw_lm_head(key, part):
    base_key = jax.random.fold_in(key, 101)
    scale = 3.0 / D ** 0.5
    table = jnp.clip(jax.random.normal(base_key, (VOC_WIN, D), jnp.float32), -6.0, 6.0) * scale
    return jnp.clip(table, -6.0, 6.0).astype(jnp.bfloat16)


def shuffled_row(row_key):
    return jax.random.permutation(row_key, CHOICES) // 4


def draw_choice_question(key, part):
    row_keys = jax.random.split(jax.random.fold_in(key, 404), N_BATCH)
    return jax.vmap(shuffled_row)(row_keys).astype(jnp.int32)


def plant(drawn, own_key, low, top_value):
    longest = drawn.shape.index(max(drawn.shape))
    spots = []
    for shift in (0, 1):
        where = [jax.random.randint(jax.random.fold_in(own_key, axis), (), 0, length) for axis, length in enumerate(drawn.shape)]
        where[longest] = (where[longest] + shift) % drawn.shape[longest]
        spots.append(tuple(where))
    return drawn.at[spots[0]].set(low).at[spots[1]].set(top_value)


def block_levels(own_key, dims, cuts, smallest, top_value):
    def one(dim, parts):
        heights = jax.random.uniform(jax.random.fold_in(jax.random.fold_in(own_key, 6), dim), (parts,), jnp.float32, smallest / len(cuts), top_value / len(cuts))
        return jnp.repeat(jnp.exp(heights), dims[dim] // parts).reshape((-1,) + (1,) * (len(dims) - dim - 1))

    level = one(*cuts[0])
    for cut in cuts[1:]:
        level = level * one(*cut)
    return level


def length_profile(amount, total, reach, slope):
    loads = [(1 << 20) // math.isqrt(grade ** slope) + 1 for grade in range(2, amount + 1)]
    surplus, given = total - reach - (amount - 1), [1] * (amount - 1)
    while surplus > 0:
        free = [i for i in range(amount - 1) if given[i] < reach]
        mass, left = sum([loads[i] for i in free]), surplus
        for i in free:
            extra = min(reach - given[i], max(1, left * loads[i] // mass), surplus)
            given[i] = given[i] + extra
            surplus = surplus - extra
    return np.array([reach] + given)


def ragged(key, count, total, bound, skew):
    if count == 2:
        one = jax.random.randint(key, (), max(1, total - bound), min(bound, total - 1) + 1)
        return jnp.stack([one, total - one])
    tallies = jnp.asarray(length_profile(count, total, bound, skew), jnp.int32)
    pairs = (count - 1) // 2
    donor, taker = tallies[1:1 + 2 * pairs:2], tallies[2:2 + 2 * pairs:2]
    margin = jnp.minimum(donor - 1, bound - taker)
    passed = jax.random.randint(jax.random.fold_in(key, 1), (pairs,), 0, 1 << 20) % (margin + 1)
    tallies = tallies.at[1:1 + 2 * pairs:2].set(donor - passed).at[2:2 + 2 * pairs:2].set(taker + passed)
    return tallies[jax.random.permutation(jax.random.fold_in(key, 2), count)]


def deal_out(key, own, number, rows, amount, top, reach, skew):
    sequence = jax.random.permutation(key, amount)
    crowded, ordinary = portions_of(amount, rows * top, reach, skew, True), portions_of(amount, rows * top, reach, skew, False)
    places = jnp.arange(amount)

    def named(sizes, rotation):
        used = int((sizes > 0).sum())
        fixed = max(1, used // 4)
        moved = fixed + (places - fixed + rotation * (used - fixed)) % max(1, amount - fixed)
        return jnp.zeros((amount,), jnp.int32).at[sequence[jnp.where(places < fixed, places, moved)]].set(jnp.asarray(sizes, jnp.int32))

    sizes = jnp.where(number % 4 == 0, named(crowded, number // 4), named(ordinary, number - number // 4 - 1))
    mixed = jax.random.permutation(jax.random.fold_in(own, 3), amount)
    source_of, sink = mixed[0:amount // 2 * 2:2], mixed[1:amount // 2 * 2:2]
    room = jnp.minimum(sizes[source_of] - 1, reach - sizes[sink]) // 2
    room = jnp.where((source_of == sequence[0]) | (sink == sequence[0]) | (sizes[sink] == 0), 0, jnp.maximum(room, 0))
    moved = jax.random.randint(jax.random.fold_in(own, 4), (amount // 2,), 0, 1 << 20) % (room + 1)
    sizes = sizes.at[source_of].add(-moved).at[sink].add(moved)
    items = jnp.searchsorted(jnp.cumsum(sizes), jnp.arange(rows * top), side="right").astype(jnp.int32)
    grid = items.reshape(top, rows).T
    grid = grid[jax.random.permutation(jax.random.fold_in(own, 1), rows)]
    rotation = jax.random.randint(jax.random.fold_in(own, 2), (rows, 1), 0, top)
    return jnp.take_along_axis(grid, (jnp.arange(top)[None, :] + rotation) % top, axis=1)


def portions_of(count, total, bound, lean, full):
    loads = [(1 << 20) // math.isqrt(standing ** lean) + 1 for standing in range(1, count + 1)]
    largest = bound if full else min(bound, max(-(-total // count), total * loads[0] // sum(loads)))
    least = 1 if total - largest >= count - 1 else 0
    holding, surplus = [largest] + [least] * (count - 1), total - largest - least * (count - 1)
    while surplus > 0:
        free = [i for i in range(1, count) if holding[i] < largest] or [i for i in range(1, count) if holding[i] < bound]
        mass, remaining = sum([loads[i] for i in free]), surplus
        for i in free:
            more = min(bound - holding[i], max(1, remaining * loads[i] // mass), surplus)
            holding[i] = holding[i] + more
            surplus = surplus - more
    return np.array(holding)


def noise(key, extent, spread, bound, cuts=(), held_as=jnp.bfloat16):
    values = jax.random.normal(key, extent, jnp.float32) * spread
    if len(cuts) > 0:
        values = block_levels(key, extent, cuts, -0.22, 0.18) * values
    return jnp.clip(values, min=-bound, max=bound).astype(held_as)


def setup_inputs(seed: int = 0) -> dict:
    splits = jax.random.split(jax.random.key(seed), 13)
    resid = draw_resid(jax.random.fold_in(splits[12], 71), 0)
    moe_gain = jnp.clip(jnp.exp(jax.random.uniform(splits[1], (D,), jnp.float32, math.log(0.25), math.log(2.5))), 0.25, 2.5)
    final_gain = jnp.clip(1.0 + 0.1 * jax.random.normal(splits[2], (D,), jnp.float32), 0.5, 1.5)
    router = noise(splits[3], (D, EXPERTS), D ** -0.5, 0.078125)
    w_gate = noise(splits[4], (EXPERTS, D, FF_WIN), D ** -0.5, 0.078125, ((0, 4), (2, 8)))
    w_up = noise(splits[5], (EXPERTS, D, FF_WIN), D ** -0.5, 0.078125, ((0, 4), (2, 8)))
    w_down = noise(splits[6], (EXPERTS, FF_WIN, D), FF_WIN ** -0.5, 0.0625, ((0, 4), (1, 8)))
    lm_head = draw_lm_head(jax.random.fold_in(splits[12], 71), 0)
    expert_ids_keys = jax.random.split(jax.random.fold_in(splits[8], 1), N_BATCH * GROUP_TOK // TOK_DEV)
    expert_ids_turns = jax.random.permutation(jax.random.fold_in(splits[8], 3), N_BATCH * GROUP_TOK // TOK_DEV)
    expert_ids = jax.vmap(lambda own, number: deal_out(jax.random.fold_in(splits[8], 2), own, number, TOK_DEV, EXPERTS, TOPK, CAP, 2))(expert_ids_keys, expert_ids_turns).reshape((N_BATCH, GROUP_TOK, TOPK))
    target_ids = plant(jax.random.randint(splits[9], (N_BATCH, GROUP_TOK), 0, VOC_WIN), jax.random.fold_in(splits[9], 1), 0, VOC_WIN - 1).astype(jnp.int32)
    choice_len = jax.vmap(lambda own: ragged(own, CHOICES, GROUP_TOK, MOSTLEN, 1))(jax.random.split(splits[10], N_BATCH)).reshape((N_BATCH, CHOICES)).astype(jnp.int32)
    choice_question = draw_choice_question(jax.random.fold_in(splits[12], 71), 0)
    return {"resid": resid, "moe_gain": moe_gain, "final_gain": final_gain, "router": router, "w_gate": w_gate, "w_up": w_up, "w_down": w_down, "lm_head": lm_head, "expert_ids": expert_ids, "target_ids": target_ids, "choice_len": choice_len, "choice_question": choice_question}


epsilon = 1e-05

def rms_scale(values, gain):
    mean_square = lax.optimization_barrier(jnp.mean(values * values, axis=-1, keepdims=True))
    return values * lax.rsqrt(mean_square + epsilon) * gain

def choice_member(lengths, positions):
    ends = jnp.cumsum(lengths, dtype=jnp.int32)
    starts = ends - lengths
    return (positions[None, :] >= starts[:, None]) & (positions[None, :] < ends[:, None])

def choice_softmax(choice_total, lengths, questions):
    average = choice_total / lengths.astype(jnp.float32)
    same_question = questions[:, None] == questions[None, :]
    question_top = lax.optimization_barrier(jnp.max(jnp.where(same_question, average[None, :], -jnp.inf), axis=1))
    raised = jnp.exp(average - question_top)
    denominator = lax.optimization_barrier(jnp.sum(jnp.where(same_question, raised[None, :], 0.0), axis=1))
    return raised / denominator

def reference(resid, moe_gain, final_gain, router, w_gate, w_up, w_down, lm_head, expert_ids, target_ids, choice_len, choice_question):
    groups, group_tokens, model_width = resid.shape
    stream = resid.reshape(-1, model_width).astype(jnp.float32)
    row_count = stream.shape[0]
    normed_in = rms_scale(stream, moe_gain).astype(jnp.bfloat16)
    router_logit = jnp.dot(normed_in, router, preferred_element_type=jnp.float32)
    route_ids = expert_ids.reshape(row_count, -1).astype(jnp.int32)
    picked = jnp.take_along_axis(router_logit, route_ids, axis=1)
    gate_weights = 1.0 / lax.optimization_barrier(jnp.sum(jnp.exp(picked[:, None, :] - picked[:, :, None]), axis=2))
    flat_ids = route_ids.reshape(-1)
    flat_gates = gate_weights.reshape(-1)
    token_of = jnp.arange(flat_ids.shape[0], dtype=jnp.int32) // route_ids.shape[1]
    slices = N_VOCAB * N_BATCH
    bound_rows = N_EXPERT * N_VOCAB * N_BATCH * CAP

    def one_expert(combined, expert):
        found = flat_ids == expert
        chosen_rows = jnp.nonzero(found, size=bound_rows, fill_value=0)[0].astype(jnp.int32)
        valid = jnp.arange(bound_rows, dtype=jnp.int32) < jnp.sum(found.astype(jnp.int32))
        tokens = token_of[chosen_rows]
        block_rows = normed_in[tokens]
        gate_part = jnp.dot(block_rows, w_gate[expert], preferred_element_type=jnp.float32)
        up_part = jnp.dot(block_rows, w_up[expert], preferred_element_type=jnp.float32)
        hidden = (jax.nn.silu(gate_part) * up_part).astype(jnp.bfloat16)
        hidden = hidden.reshape(bound_rows, slices, -1)
        down_parts = w_down[expert].reshape(slices, -1, model_width)

        def add_slice(running, slice_index):
            part = jnp.dot(hidden[:, slice_index], down_parts[slice_index], preferred_element_type=jnp.float32).astype(jnp.bfloat16)
            part = lax.optimization_barrier(part)
            return (running + part.astype(jnp.float32), None)
        running, _ = lax.scan(add_slice, jnp.zeros((bound_rows, model_width), jnp.float32), jnp.arange(slices, dtype=jnp.int32))
        expert_out = lax.optimization_barrier(running.astype(jnp.bfloat16)).astype(jnp.float32)
        weight = jnp.where(valid, flat_gates[chosen_rows], 0.0)
        return (combined.at[tokens].add(weight[:, None] * expert_out), None)
    combined, _ = lax.scan(one_expert, jnp.zeros((row_count, model_width), jnp.float32), jnp.arange(EXPERTS, dtype=jnp.int32))
    mixed_rows = stream + combined
    normed_out = rms_scale(mixed_rows, final_gain).astype(jnp.bfloat16)
    logits = lax.dot_general(normed_out, lm_head, (((1,), (1,)), ((), ())), preferred_element_type=jnp.float32)
    largest = lax.optimization_barrier(jnp.max(logits, axis=1))
    log_total = largest + jnp.log(lax.optimization_barrier(jnp.sum(jnp.exp(logits - largest[:, None]), axis=1)))
    target_logit = jnp.take_along_axis(logits, target_ids.reshape(-1, 1).astype(jnp.int32), axis=1)[:, 0]
    token_logprob = (target_logit - log_total).reshape(groups, group_tokens)
    positions = jnp.arange(group_tokens, dtype=jnp.int32)

    def group_probs(logprob_row, lengths, questions):
        member = choice_member(lengths, positions)
        choice_total = lax.optimization_barrier(jnp.sum(jnp.where(member, logprob_row[None, :], 0.0), axis=1))
        return choice_softmax(choice_total, lengths, questions)
    choice_prob = jax.vmap(group_probs)(token_logprob, choice_len, choice_question)
    return (token_logprob, choice_prob)
```

```python
import functools

import jax
import jax.numpy as jnp
from jax import lax
from jax.experimental import pallas as pl
from jax.experimental.pallas import tpu as pltpu
from jax.sharding import PartitionSpec as P

epsilon = 1e-05


def joined(array, axis, combine):
    everything = jax.tree.map(lambda part: lax.all_gather(part, axis), array)
    leading = jax.tree.map(lambda part: part[0], everything)

    def lap(k, so_far):
        return combine(so_far, jax.tree.map(lambda part: part[k], everything))

    return lax.fori_loop(1, lax.axis_size(axis), lap, leading)


def rms_scale(values, gain):
    mean_square = jnp.mean(values * values, axis=-1, keepdims=True)
    return values * lax.rsqrt(mean_square + epsilon) * gain


def route_gates(router_logit, route_ids):
    expert_count = router_logit.shape[1]
    matches = route_ids[:, :, None] == jnp.arange(expert_count, dtype=jnp.int32)[None, None, :]
    picked = jnp.sum(jnp.where(matches, router_logit[:, None, :], 0.0), axis=2)
    return 1.0 / jnp.sum(jnp.exp(picked[:, None, :] - picked[:, :, None]), axis=2)


def expand_rows(block_rows, gate_cols, up_cols):
    gate_part = jnp.dot(block_rows, gate_cols, preferred_element_type=jnp.float32)
    up_part = jnp.dot(block_rows, up_cols, preferred_element_type=jnp.float32)
    return (jax.nn.silu(gate_part) * up_part).astype(jnp.bfloat16)


def choice_member(lengths, positions):
    ends = jnp.cumsum(lengths, dtype=jnp.int32)
    starts = ends - lengths
    return (positions[None, :] >= starts[:, None]) & (positions[None, :] < ends[:, None])


def choice_softmax(choice_total, lengths, questions):
    average = choice_total / lengths.astype(jnp.float32)
    same_question = questions[:, None] == questions[None, :]
    question_top = jnp.max(jnp.where(same_question, average[None, :], -jnp.inf), axis=1)
    raised = jnp.exp(average - question_top)
    denominator = jnp.sum(jnp.where(same_question, raised[None, :], 0.0), axis=1)
    return raised / denominator


def merge_stats(first, second):
    top_value = jnp.maximum(first[0], second[0])
    summed = first[1] * jnp.exp(first[0] - top_value) + second[1] * jnp.exp(second[0] - top_value)
    return (top_value, summed, first[2] + second[2])


def on_device(
    resid,
    moe_gain,
    final_gain,
    router,
    w_gate,
    w_up,
    w_down,
    lm_head,
    expert_ids,
    target_ids,
    choice_len,
    choice_question,
):
    stream = resid[0].astype(jnp.float32)
    token_count, model_width = stream.shape
    normed_in = rms_scale(stream, moe_gain).astype(jnp.bfloat16)
    router_logit = jnp.dot(normed_in, router, preferred_element_type=jnp.float32)
    route_ids = expert_ids[0]
    route_count = route_ids.shape[1]
    gate_weights = route_gates(router_logit, route_ids)
    expert_count = lax.axis_size("expert")
    bucket_size = max(2, (token_count * route_count + expert_count - 1) // expert_count + 1)
    flat_ids = route_ids.reshape(-1)
    expert_match = (flat_ids[:, None] == jnp.arange(expert_count, dtype=jnp.int32)[None, :]).astype(
        jnp.int32
    )
    earlier = jnp.cumsum(expert_match, axis=0, dtype=jnp.int32) - expert_match
    slot_index = flat_ids * bucket_size + jnp.sum(earlier * expert_match, axis=1)
    slot_match = (
        slot_index[:, None] == jnp.arange(expert_count * bucket_size, dtype=jnp.int32)[None, :]
    ).astype(jnp.float32)
    slot_match = slot_match.reshape(token_count, route_count, -1)
    dispatch = jnp.sum(slot_match, axis=1).astype(jnp.bfloat16)
    combine_weights = jnp.sum(slot_match * gate_weights[:, :, None], axis=1)
    buckets = lax.dot_general(
        dispatch, normed_in, (((0,), (0,)), ((), ())), preferred_element_type=jnp.float32
    )
    buckets = buckets.astype(jnp.bfloat16).reshape(expert_count, bucket_size, model_width)
    gate_cols = w_gate[0]
    up_cols = w_up[0]
    down_rows = w_down[0]
    arrived = lax.all_to_all(buckets, "expert", split_axis=0, concat_axis=0, tiled=True).reshape(
        -1, model_width
    )
    hidden = expand_rows(
        lax.all_gather(arrived, ("vocab", "batch"), axis=0, tiled=True), gate_cols, up_cols
    )
    expert_sum = lax.psum_scatter(
        jnp.dot(hidden, down_rows, preferred_element_type=jnp.float32).astype(jnp.bfloat16),
        ("vocab", "batch"),
        scatter_dimension=0,
        tiled=True,
    )
    outgoing = expert_sum.reshape(expert_count, bucket_size, model_width)
    returned = lax.all_to_all(outgoing, "expert", split_axis=0, concat_axis=0, tiled=True)
    returned_rows = returned.reshape(-1, model_width).astype(jnp.float32)
    mixed_rows = stream + jnp.dot(combine_weights, returned_rows, precision=lax.Precision.HIGHEST)
    normed_out = rms_scale(mixed_rows, final_gain).astype(jnp.bfloat16)
    head_index = lax.axis_index(("expert", "vocab"))
    vocab_share = lm_head.shape[0]
    vocab_ids = jnp.arange(vocab_share, dtype=jnp.int32) + head_index * vocab_share
    targets = target_ids[0]
    group_tokens = targets.shape[0]
    logits = lax.dot_general(
        lax.all_gather(normed_out, ("expert", "vocab"), axis=0, tiled=True),
        lm_head,
        (((1,), (1,)), ((), ())),
        preferred_element_type=jnp.float32,
    )
    block_top = jnp.max(logits, axis=1)
    block_sum = jnp.sum(jnp.exp(logits - block_top[:, None]), axis=1)
    block_hit = jnp.sum(jnp.where(targets[:, None] == vocab_ids[None, :], logits, 0.0), axis=1)
    fresh = (block_top, block_sum, block_hit)
    largest, spread_sum, chosen = tuple((fresh[slot] for slot in range(3)))
    lengths = choice_len[0]
    questions = choice_question[0]
    own_first = head_index * token_count
    group_positions = jnp.arange(group_tokens, dtype=jnp.int32)
    best, summed, target_sum = joined(
        (largest, spread_sum, chosen), ("expert", "vocab"), merge_stats
    )
    group_logprob = target_sum - (best + jnp.log(summed))
    choice_total = jnp.sum(
        jnp.where(choice_member(lengths, group_positions), group_logprob[None, :], 0.0), axis=1
    )
    own_logprob = lax.dynamic_slice_in_dim(group_logprob, own_first, token_count, 0)
    choice_prob = choice_softmax(choice_total, lengths, questions)
    return (own_logprob.reshape(1, -1), choice_prob.reshape(1, -1))


MESH = pl.DeviceIdType.MESH
VMEM_BYTES = 67043328
CHUNKS = 6


def greet(partners):
    barrier = pltpu.get_barrier_semaphore()
    for partner in partners:
        pl.semaphore_signal(barrier, inc=1, device_id=partner, device_id_type=MESH)
    pl.semaphore_wait(barrier, len(partners))


def push(src, dst, send_sem, recv_sem, partner):
    return pltpu.make_async_remote_copy(
        src_ref=src,
        dst_ref=dst,
        send_sem=send_sem,
        recv_sem=recv_sem,
        device_id=partner,
        device_id_type=MESH,
    )


SKEW_MIX = 5
SKEW_FORWARD = 7
SKEW_HEAD = 8


def row_cap(ne, tokens, routes):
    return max(2, (tokens * routes + ne - 1) // ne + 1)


def wide(value):
    return value.astype(jnp.float32)


def iota(shape, axis):
    return lax.broadcasted_iota(jnp.int32, shape, axis)


def as_column(row, count):
    eye = iota((count, row.shape[1]), 0) == iota((count, row.shape[1]), 1)
    return jnp.sum(jnp.where(eye, row, 0.0), axis=1, keepdims=True)


def as_row(column, lanes):
    count = column.shape[0]
    eye = iota((count, lanes), 0) == iota((count, lanes), 1)
    return jnp.sum(jnp.where(eye, column, 0.0), axis=0, keepdims=True)


def fused_kernel(
    ne,
    nv,
    nb,
    cap,
    resid_ref,
    moe_gain_ref,
    final_gain_ref,
    router_ref,
    ids_ref,
    target_ref,
    length_ref,
    question_ref,
    wg_hbm,
    wu_hbm,
    wd_hbm,
    head_hbm,
    logprob_ref,
    prob_ref,
    big,
    wd,
    zout,
    zin,
    xs,
    xl,
    g_acc,
    u_acc,
    hid,
    pm,
    po,
    rpair,
    sy,
    ry,
    sx,
    rx,
    zs,
    zo,
    ys,
    logits,
    scales,
    stats,
    w_sem,
    wd_sem,
    h_sem,
    z_send,
    z_recv,
    c_send,
    c_recv,
    m_send,
    m_recv,
    r_send,
    r_recv,
    o_send,
    o_recv,
    y_send,
    y_recv,
    s_send,
    s_recv,
):
    e, v, b = lax.axis_index("expert"), lax.axis_index("vocab"), lax.axis_index("batch")
    core = lax.rem(b, 2)
    other = 1 - core
    tokens, width = resid_ref.shape
    half = width // 2
    n = CHUNKS
    cw = half // n
    chip_rows = ne * 2 * cap
    tiles = chip_rows // 8
    rows = 4 * chip_rows
    hidden = hid.shape[1]
    share = head_hbm.shape[0]
    block = big.shape[1]
    peers = ne * nv
    me = e * nv + v
    across = (e, 1 - v, b)
    along = (e, v, lax.rem(b + 2, 4))
    turned = b + 1 - 2 * core
    mate = (e, v, turned)
    bf16 = jnp.bfloat16

    def cols(j):
        return pl.ds(j * cw, cw)

    column = []
    for k in range(ne):
        for s in range(2):
            if k + s > 0:
                to = lax.rem(e + k, ne)
                column.append((k * 2 + s, to, other if s else core, (to, v, turned if s else b)))

    def at(k):
        p = lax.rem(me + k, peers)
        return (p // nv, lax.rem(p, nv), b)

    weight_loads = {}
    for j in range(n):
        for which, source in enumerate((wg_hbm, wu_hbm)):
            for h in range(2):
                first = h * half + j * cw
                weight_loads[j, which, h] = pltpu.make_async_copy(
                    source.at[0, pl.ds(first, cw)],
                    big.at[pl.ds(which * width + first, cw)],
                    w_sem.at[j, which * 2 + h],
                )
                weight_loads[j, which, h].start()
    down_load = pltpu.make_async_copy(wd_hbm.at[0], wd, wd_sem.at[0])
    down_load.start()

    barrier = pltpu.get_barrier_semaphore()
    greeted = [where for _, _, _, where in column]
    greeted += [(lax.rem(e + k, ne), 1 - v, b) for k in range(ne)] + [along]
    for partner in greeted:
        pl.semaphore_signal(barrier, inc=1, device_id=partner, device_id_type=MESH)

    stream = wide(resid_ref[...])
    mean_square = jnp.sum(stream * stream, axis=1, keepdims=True) * (1.0 / width)
    normed = wide((stream * lax.rsqrt(mean_square + epsilon) * moe_gain_ref[...]).astype(bf16))
    ids = wide(ids_ref[...])
    first_row, second_row = ids[0:1, :], ids[1:2, :]
    expert_of = wide(lax.shift_right_logical(iota((ne * 8, tokens), 0), 3))
    slot_of = wide(iota((ne * 8, tokens), 0) & 7)
    named = (first_row == expert_of) | (second_row == expert_of)
    before = jnp.where(iota((tokens, tokens), 0) < iota((tokens, tokens), 1), 1.0, 0.0)
    rank = jnp.dot(jnp.where(named, 1.0, 0.0), before, preferred_element_type=jnp.float32)
    dispatch = jnp.where(named & (rank == slot_of), 1.0, 0.0)
    for h in range(2):
        for j in range(n):
            first = h * half + j * cw
            routed = jnp.dot(
                dispatch, normed[:, first : first + cw], preferred_element_type=jnp.float32
            )
            zout[h, :, :, cols(j)] = routed.reshape(ne, 8, cw).astype(bf16)
    pl.semaphore_wait(barrier, len(greeted))

    z_copies = {}
    for j in range(n):
        for slot, to, ct, where in column:
            z_copies[j, slot] = push(
                zout.at[ct, to, :, cols(j)],
                zin.at[e, core, :, cols(j)],
                z_send.at[j, slot],
                z_recv.at[j, slot],
                where,
            )
            z_copies[j, slot].start()
    zin[e, core] = zout[core, e]

    first_id, second_id = as_column(first_row, tokens), as_column(second_row, tokens)
    expert_lane = wide(lax.shift_right_logical(iota((tokens, ne * 8), 1), 3))
    slot_lane = wide(iota((tokens, ne * 8), 1) & 7)
    first_here, second_here = first_id == expert_lane, second_id == expert_lane
    after = jnp.where(iota((tokens, tokens), 1) < iota((tokens, tokens), 0), 1.0, 0.0)
    rank = jnp.dot(
        after, jnp.where(first_here | second_here, 1.0, 0.0), preferred_element_type=jnp.float32
    )
    first_logit = jnp.zeros((tokens, 1), jnp.float32)
    second_logit = jnp.zeros((tokens, 1), jnp.float32)
    for k in range(ne):
        router_logit = jnp.sum(normed * wide(router_ref[k : k + 1, :]), axis=1, keepdims=True)
        first_logit = first_logit + jnp.where(first_id == k, router_logit, 0.0)
        second_logit = second_logit + jnp.where(second_id == k, router_logit, 0.0)
    first_gate = 1.0 / (1.0 + jnp.exp(second_logit - first_logit))
    second_gate = 1.0 / (1.0 + jnp.exp(first_logit - second_logit))
    combine = jnp.where(
        rank == slot_lane,
        jnp.where(first_here, first_gate, jnp.where(second_here, second_gate, 0.0)),
        0.0,
    )
    coarse = wide(combine.astype(bf16))
    combine = jnp.concatenate([coarse, combine - coarse], axis=0).astype(bf16)

    def packing(shape, packed_axis):
        padded = iota(shape, 1 - packed_axis)
        slot = padded & 7
        place = lax.shift_right_logical(padded, 3) * cap + slot
        return jnp.where((slot < cap) & (place == iota(shape, packed_axis)), 1.0, 0.0).astype(bf16)

    pack = packing((chip_rows, ne * 16), 0)
    unpack = packing((ne * 16, chip_rows), 1)

    def plane_push(src_slot, dst_slot, j, partner):
        return push(
            xs.at[src_slot, core, :, :, cols(j)],
            xs.at[dst_slot, core, :, :, cols(j)],
            c_send.at[j, dst_slot],
            c_recv.at[j, dst_slot],
            partner,
        )

    c_copies, m_copies = {}, {}

    def mate_push(slot, j):
        m_copies[j, slot] = push(
            xs.at[slot, core, :, :, cols(j)],
            xs.at[slot, core, :, :, cols(j)],
            m_send.at[j, slot],
            m_recv.at[j, slot],
            mate,
        )
        m_copies[j, slot].start()

    def pack_rows(j):
        for slot, _, _, _ in column:
            z_copies[j, slot].wait_recv()
        padded = wide(zin[:, :, :, cols(j)]).reshape(ne * 16, cw).astype(bf16)
        packed = jnp.dot(pack, padded, preferred_element_type=jnp.float32)
        xs[0, core, :, :, cols(j)] = packed.reshape(tiles, 8, cw).astype(bf16)
        for slot, partner in ((1, across), (2, along)):
            c_copies[j, slot] = plane_push(0, slot, j, partner)
            c_copies[j, slot].start()
        mate_push(0, j)

    def relay(j):
        source, partner = (1, along) if j % 2 == 0 else (2, across)
        c_copies[j, source].wait_recv()
        c_copies[j, 3] = plane_push(source, 3, j, partner)
        c_copies[j, 3].start()
        mate_push(source, j)
        c_copies[j, 3 - source].wait_recv()
        mate_push(3 - source, j)

    def corner(j):
        c_copies[j, 3].wait_recv()
        mate_push(3, j)

    tile = min(256, hidden)

    def expand(j):
        for slot in range(4):
            m_copies[j, slot].wait_recv()
        for h in range(2):
            xl[h] = wide(xs[:, h, :, :, cols(j)]).reshape(rows, cw).astype(bf16)
        for which in range(2):
            for h in range(2):
                weight_loads[j, which, h].wait()

        @pl.loop(0, hidden // tile)
        def _(i):
            where = pl.ds(pl.multiple_of(i * tile, tile), tile)

            def product(which):
                low = which * width + j * cw
                return jnp.dot(
                    xl[0], big[low : low + cw, where], preferred_element_type=jnp.float32
                ) + jnp.dot(
                    xl[1],
                    big[low + half : low + half + cw, where],
                    preferred_element_type=jnp.float32,
                )

            g, u = product(0), product(1)
            if j > 0:
                g, u = g + g_acc[:, where], u + u_acc[:, where]
            if j < n - 1:
                g_acc[:, where] = g
                u_acc[:, where] = u
            else:
                hid[:, where] = (g / (1.0 + jnp.exp(-g)) * u).astype(bf16)

    for i in range(n + 3):
        for skew, stage in enumerate((pack_rows, relay, corner, expand)):
            if 0 <= i - skew < n:
                stage(i - skew)

    head_loads = []
    per_half = half // block
    for q in range(per_half):
        for h in range(2):
            place = h * per_half + q
            head_loads.append(
                pltpu.make_async_copy(
                    head_hbm.at[:, pl.ds(place * block, block)],
                    big.at[pl.ds(place * share, share)],
                    h_sem.at[place],
                )
            )
            head_loads[-1].start()
    down_load.wait()

    rp, yc, xc, zc, gz, gx = {}, {}, {}, {}, {}, {}

    def down(j):
        def product(side):
            where = pl.ds(pl.multiple_of(side * half + j * cw, 128), cw)
            return jnp.dot(hid[...], wd[:, where], preferred_element_type=jnp.float32)

        pm[:, :, :, cols(j)] = product(other).reshape(4, tiles, 8, cw).astype(bf16)
        rp[j] = push(
            pm.at[:, :, :, cols(j)], rpair.at[:, :, :, cols(j)], r_send.at[j, 0], r_recv.at[j, 0], mate
        )
        rp[j].start()
        po[:, cols(j)] = product(core)

    def pair_sum(j):
        rp[j].wait_recv()
        total = po[:, cols(j)] + wide(rpair[:, :, :, cols(j)]).reshape(rows, cw)
        sy[:, :, :, cols(j)] = total[2 * chip_rows :].reshape(2, tiles, 8, cw).astype(bf16)
        yc[j] = push(
            sy.at[:, :, :, cols(j)], ry.at[:, :, :, cols(j)], r_send.at[j, 1], r_recv.at[j, 1], along
        )
        yc[j].start()
        po[0 : 2 * chip_rows, cols(j)] = total[: 2 * chip_rows]

    def y_sum(j):
        yc[j].wait_recv()
        total = po[0 : 2 * chip_rows, cols(j)] + wide(ry[:, :, :, cols(j)]).reshape(2 * chip_rows, cw)
        sx[:, :, cols(j)] = total[chip_rows:].reshape(tiles, 8, cw).astype(bf16)
        xc[j] = push(
            sx.at[:, :, cols(j)], rx.at[:, :, cols(j)], r_send.at[j, 2], r_recv.at[j, 2], across
        )
        xc[j].start()
        po[0:chip_rows, cols(j)] = total[:chip_rows]

    def x_sum(j):
        xc[j].wait_recv()
        total = po[0:chip_rows, cols(j)] + wide(rx[:, :, cols(j)]).reshape(chip_rows, cw)
        padded = jnp.dot(unpack, total.astype(bf16), preferred_element_type=jnp.float32)
        zs[:, :, :, cols(j)] = padded.reshape(ne, 2, 8, cw).astype(bf16)
        for slot, to, ct, where in column:
            zc[j, slot] = push(
                zs.at[to, ct, :, cols(j)],
                zo.at[e, core, :, cols(j)],
                o_send.at[j, slot],
                o_recv.at[j, slot],
                where,
            )
            zc[j, slot].start()
        zo[e, core, :, cols(j)] = zs[e, core, :, cols(j)]

    squares = [jnp.zeros((tokens, 1), jnp.float32)]

    def mix(j):
        for slot, _, _, _ in column:
            zc[j, slot].wait_recv()
        for h in range(2):
            first = h * half + j * cw
            returned = wide(zo[:, h, :, cols(j)]).reshape(ne * 8, cw).astype(bf16)
            weighted = jnp.dot(combine, returned, preferred_element_type=jnp.float32)
            mixed = wide(resid_ref[:, first : first + cw]) + (weighted[:tokens] + weighted[tokens:])
            squares[0] = squares[0] + jnp.sum(mixed * mixed, axis=1, keepdims=True)
            ys[me, j, h] = (mixed * final_gain_ref[:, first : first + cw]).astype(bf16)
        for k in range(1, ne):
            gz[j, k] = push(
                ys.at[me, j],
                ys.at[me, j],
                y_send.at[j, k],
                y_recv.at[j, k],
                (lax.rem(e + k, ne), v, b),
            )
            gz[j, k].start()
        turn(j, 0)

    def turn(j, k):
        slot = lax.rem(e + ne - k, ne) * nv + v
        gx[j, k] = push(
            ys.at[slot, j], ys.at[slot, j], y_send.at[j, ne + k], y_recv.at[j, ne + k], across
        )
        gx[j, k].start()

    def forward(j):
        for k in (1, 3, 2) if ne == 4 else range(1, ne):
            gz[j, k].wait_recv()
            turn(j, k)

    head_tile = min(256, share)

    def head(j):
        for k in range(ne):
            gx[j, k].wait_recv()
        if (j * cw) % block == 0:
            for h in range(2):
                head_loads[(j * cw) // block * 2 + h].wait()
        sides = []
        for h in range(2):
            sides.append(wide(ys[:, j, h]).reshape(peers * tokens, cw).astype(bf16))
        left = (j * cw) % block
        low = (j * cw) // block * share

        @pl.loop(0, share // head_tile)
        def _(i):
            first = pl.multiple_of(i * head_tile, head_tile)
            found = 0.0
            for h in range(2):
                found = found + lax.dot_general(
                    sides[h],
                    big[pl.ds(low + h * per_half * share + first, head_tile), left : left + cw],
                    (((1,), (1,)), ((), ())),
                    preferred_element_type=jnp.float32,
                )
            if j > 0:
                found = found + logits[:, pl.ds(first, head_tile)]
            logits[:, pl.ds(first, head_tile)] = found

    small = []

    def share_scale(j):
        if j < n - 1:
            return
        scale = lax.rsqrt(squares[0] * (1.0 / width) + epsilon)
        scales[me] = jnp.broadcast_to(scale, (tokens, 128))
        for k in range(1, peers):
            small.append(
                push(scales.at[me], scales.at[me], s_send.at[0, k], s_recv.at[0, k], at(k))
            )
            small[-1].start()

    stages = (
        (0, down),
        (1, pair_sum),
        (2, y_sum),
        (3, x_sum),
        (SKEW_MIX, mix),
        (SKEW_MIX, share_scale),
        (SKEW_FORWARD, forward),
        (SKEW_HEAD, head),
    )
    for i in range(n + SKEW_HEAD):
        for skew, stage in stages:
            if 0 <= i - skew < n:
                stage(i - skew)

    for copy in small:
        copy.wait_recv()
    group = peers * tokens
    lanes = 128
    scaled = logits[...] * scales[...].reshape(group, lanes)[:, 0:1]
    targets = as_column(wide(target_ref[...]), group)
    vocab_ids = wide(iota((group, share), 1) + me * share)
    top = jnp.max(scaled, axis=1, keepdims=True)
    total = jnp.sum(jnp.exp(scaled - top), axis=1, keepdims=True)
    hit = jnp.sum(jnp.where(vocab_ids == targets, scaled, 0.0), axis=1, keepdims=True)
    line = iota((8, lanes), 0)
    stats[me] = jnp.where(
        line == 0,
        as_row(top, lanes),
        jnp.where(line == 1, as_row(total, lanes), jnp.where(line == 2, as_row(hit, lanes), 0.0)),
    )
    sends = [
        push(stats.at[me], stats.at[me], s_send.at[1, k], s_recv.at[1, k], at(k))
        for k in range(1, peers)
    ]
    for copy in sends:
        copy.start()

    choices = length_ref.shape[1]
    lengths_row, questions_row = wide(length_ref[...]), wide(question_ref[...])
    lengths, questions = as_column(lengths_row, choices), as_column(questions_row, choices)
    square = (choices, choices)
    ends = jnp.sum(jnp.where(iota(square, 1) <= iota(square, 0), lengths_row, 0.0), axis=1, keepdims=True)
    place = wide(iota((choices, lanes), 1))
    member = (place >= ends - lengths) & (place < ends)
    same = questions == questions_row

    for copy in sends:
        copy.wait_recv()
    every = stats[...]
    best = jnp.max(every[:, 0:1, :], axis=0)
    summed = jnp.sum(every[:, 1:2, :] * jnp.exp(every[:, 0:1, :] - best[None]), axis=0)
    chosen = jnp.sum(every[:, 2:3, :], axis=0)
    used = iota((1, lanes), 1) < group
    logprob = jnp.where(used, chosen - (best + jnp.log(jnp.where(used, summed, 1.0))), 0.0)
    own = jnp.sum(
        jnp.where(iota((tokens, lanes), 1) == iota((tokens, lanes), 0) + me * tokens, logprob, 0.0),
        axis=1,
        keepdims=True,
    )
    logprob_ref[...] = as_row(own, tokens)
    average = jnp.sum(jnp.where(member, logprob, 0.0), axis=1, keepdims=True) / lengths
    question_top = jnp.max(
        jnp.where(same, as_row(average, choices), -jnp.inf), axis=1, keepdims=True
    )
    raised = jnp.exp(average - question_top)
    denominator = jnp.sum(jnp.where(same, as_row(raised, choices), 0.0), axis=1, keepdims=True)
    prob_ref[...] = as_row(raised / denominator, choices)

    for copies in (z_copies, c_copies, m_copies, rp, yc, xc, zc, gz, gx):
        for copy in copies.values():
            copy.wait_send()
    for copy in small + sends:
        copy.wait_send()


def fused_call(sizes, resid, moe_gain, final_gain, router, ids, targets, lengths, questions, *weights):
    ne, nv, nb = sizes
    tokens, width = resid.shape
    w_gate, _, _, lm_head = weights
    hidden = w_gate.shape[2]
    share = lm_head.shape[0]
    cap = row_cap(ne, tokens, ids.shape[0])
    half = width // 2
    tiles = ne * 2 * cap // 8
    rows = 4 * tiles * 8
    peers = ne * nv
    n = CHUNKS
    cw = half // n
    bf16, f32 = jnp.bfloat16, jnp.float32
    dma = pltpu.SemaphoreType.DMA
    vmem = pltpu.VMEM
    vm = pl.BlockSpec(memory_space=pltpu.VMEM)
    anywhere = pl.BlockSpec(memory_space=pl.ANY)
    return pl.pallas_call(
        functools.partial(fused_kernel, ne, nv, nb, cap),
        out_shape=(
            jax.ShapeDtypeStruct((1, tokens), f32),
            jax.ShapeDtypeStruct((1, lengths.shape[1]), f32),
        ),
        in_specs=[vm] * 8 + [anywhere] * 4,
        out_specs=(vm, vm),
        scratch_shapes=[
            vmem((2 * width, hidden), bf16),
            vmem((hidden, width), bf16),
            vmem((2, ne, 8, half), bf16),
            vmem((ne, 2, 8, half), bf16),
            vmem((4, 2, tiles, 8, half), bf16),
            vmem((2, rows, cw), bf16),
            vmem((rows, hidden), f32),
            vmem((rows, hidden), f32),
            vmem((rows, hidden), bf16),
            vmem((4, tiles, 8, half), bf16),
            vmem((rows, half), f32),
            vmem((4, tiles, 8, half), bf16),
            vmem((2, tiles, 8, half), bf16),
            vmem((2, tiles, 8, half), bf16),
            vmem((tiles, 8, half), bf16),
            vmem((tiles, 8, half), bf16),
            vmem((ne, 2, 8, half), bf16),
            vmem((ne, 2, 8, half), bf16),
            vmem((peers, n, 2, 8, cw), bf16),
            vmem((peers * tokens, share), f32),
            vmem((peers, tokens, 128), f32),
            vmem((peers, 8, 128), f32),
            dma((n, 4)),
            dma((1,)),
            dma((width // hidden,)),
            dma((n, 2 * ne)),
            dma((n, 2 * ne)),
            dma((n, 4)),
            dma((n, 4)),
            dma((n, 4)),
            dma((n, 4)),
            dma((n, 3)),
            dma((n, 3)),
            dma((n, 2 * ne)),
            dma((n, 2 * ne)),
            dma((n, 2 * ne)),
            dma((n, 2 * ne)),
            dma((2, peers)),
            dma((2, peers)),
        ],
        compiler_params=pltpu.CompilerParams(
            collective_id=0, has_side_effects=True, vmem_limit_bytes=VMEM_BYTES - 1024 * 1024
        ),
        name="fused",
    )(resid, moe_gain, final_gain, router, ids, targets, lengths, questions, *weights)


def kernel_fits(sizes, *arrays):
    ne, nv, nb = sizes
    resid, w_gate, lm_head, ids = arrays[0], arrays[4], arrays[7], arrays[8]
    tokens, width = resid.shape[1:]
    hidden = w_gate.shape[2]
    share = lm_head.shape[0]
    cap = row_cap(ne, tokens, ids.shape[2])
    rows = 8 * ne * cap
    need = 2 * (3 * width * hidden + rows * (4 * width + 6 * hidden) + 8 * ne * 8 * width)
    return (
        nv == 2
        and nb == 4
        and tokens == 8
        and ids.shape[2] == 2
        and cap <= 8
        and ne * 2 * cap % 8 == 0
        and width % (2 * hidden) == 0
        and width % (2 * CHUNKS * 128) == 0
        and hidden % (width // 2 // CHUNKS) == 0
        and hidden % 256 == 0
        and share == 2 * hidden
        and ne * nv * tokens <= 128
        and need < VMEM_BYTES - 4 * 1024 * 1024
    )


def on_device_kernel(
    sizes,
    resid,
    moe_gain,
    final_gain,
    router,
    w_gate,
    w_up,
    w_down,
    lm_head,
    expert_ids,
    target_ids,
    choice_len,
    choice_question,
):
    return fused_call(
        sizes,
        resid[0],
        moe_gain.reshape(1, -1),
        final_gain.reshape(1, -1),
        router.T,
        expert_ids[0].T,
        target_ids,
        choice_len,
        choice_question,
        w_gate,
        w_up,
        w_down,
        lm_head,
    )


def either(sizes, *arrays):
    if kernel_fits(sizes, *arrays):
        return on_device_kernel(sizes, *arrays)
    return on_device(*arrays)


def solution(mesh):
    sizes = tuple(mesh.shape[axis] for axis in ("expert", "vocab", "batch"))
    return jax.shard_map(
        functools.partial(either, sizes),
        mesh=mesh,
        in_specs=(
            P("batch", ("expert", "vocab"), None),
            P(),
            P(),
            P(),
            P("expert", None, ("vocab", "batch")),
            P("expert", None, ("vocab", "batch")),
            P("expert", ("vocab", "batch"), None),
            P(("expert", "vocab"), None),
            P("batch", ("expert", "vocab"), None),
            P("batch", None),
            P("batch", None),
            P("batch", None),
        ),
        out_specs=(P("batch", ("expert", "vocab")), P("batch", None)),
        check_vma=False,
    )
```

```python
import functools

import jax
import jax.numpy as jnp
from jax import lax
from jax.experimental import pallas as pl
from jax.experimental.pallas import tpu as pltpu
from jax.sharding import PartitionSpec as P

epsilon = 1e-05


def joined(array, axis, combine):
    everything = jax.tree.map(lambda part: lax.all_gather(part, axis), array)
    leading = jax.tree.map(lambda part: part[0], everything)

    def lap(k, so_far):
        return combine(so_far, jax.tree.map(lambda part: part[k], everything))

    return lax.fori_loop(1, lax.axis_size(axis), lap, leading)


def rms_scale(values, gain):
    mean_square = jnp.mean(values * values, axis=-1, keepdims=True)
    return values * lax.rsqrt(mean_square + epsilon) * gain


def route_gates(router_logit, route_ids):
    expert_count = router_logit.shape[1]
    matches = route_ids[:, :, None] == jnp.arange(expert_count, dtype=jnp.int32)[None, None, :]
    picked = jnp.sum(jnp.where(matches, router_logit[:, None, :], 0.0), axis=2)
    return 1.0 / jnp.sum(jnp.exp(picked[:, None, :] - picked[:, :, None]), axis=2)


def expand_rows(block_rows, gate_cols, up_cols):
    gate_part = jnp.dot(block_rows, gate_cols, preferred_element_type=jnp.float32)
    up_part = jnp.dot(block_rows, up_cols, preferred_element_type=jnp.float32)
    return (jax.nn.silu(gate_part) * up_part).astype(jnp.bfloat16)


def choice_member(lengths, positions):
    ends = jnp.cumsum(lengths, dtype=jnp.int32)
    starts = ends - lengths
    return (positions[None, :] >= starts[:, None]) & (positions[None, :] < ends[:, None])


def choice_softmax(choice_total, lengths, questions):
    average = choice_total / lengths.astype(jnp.float32)
    same_question = questions[:, None] == questions[None, :]
    question_top = jnp.max(jnp.where(same_question, average[None, :], -jnp.inf), axis=1)
    raised = jnp.exp(average - question_top)
    denominator = jnp.sum(jnp.where(same_question, raised[None, :], 0.0), axis=1)
    return raised / denominator


def merge_stats(first, second):
    top_value = jnp.maximum(first[0], second[0])
    summed = first[1] * jnp.exp(first[0] - top_value) + second[1] * jnp.exp(second[0] - top_value)
    return (top_value, summed, first[2] + second[2])


def on_device(
    resid,
    moe_gain,
    final_gain,
    router,
    w_gate,
    w_up,
    w_down,
    lm_head,
    expert_ids,
    target_ids,
    choice_len,
    choice_question,
):
    stream = resid[0].astype(jnp.float32)
    token_count, model_width = stream.shape
    normed_in = rms_scale(stream, moe_gain).astype(jnp.bfloat16)
    router_logit = jnp.dot(normed_in, router, preferred_element_type=jnp.float32)
    route_ids = expert_ids[0]
    route_count = route_ids.shape[1]
    gate_weights = route_gates(router_logit, route_ids)
    expert_count = lax.axis_size("expert")
    bucket_size = max(2, (token_count * route_count + expert_count - 1) // expert_count + 1)
    flat_ids = route_ids.reshape(-1)
    expert_match = (flat_ids[:, None] == jnp.arange(expert_count, dtype=jnp.int32)[None, :]).astype(
        jnp.int32
    )
    earlier = jnp.cumsum(expert_match, axis=0, dtype=jnp.int32) - expert_match
    slot_index = flat_ids * bucket_size + jnp.sum(earlier * expert_match, axis=1)
    slot_match = (
        slot_index[:, None] == jnp.arange(expert_count * bucket_size, dtype=jnp.int32)[None, :]
    ).astype(jnp.float32)
    slot_match = slot_match.reshape(token_count, route_count, -1)
    dispatch = jnp.sum(slot_match, axis=1).astype(jnp.bfloat16)
    combine_weights = jnp.sum(slot_match * gate_weights[:, :, None], axis=1)
    buckets = lax.dot_general(
        dispatch, normed_in, (((0,), (0,)), ((), ())), preferred_element_type=jnp.float32
    )
    buckets = buckets.astype(jnp.bfloat16).reshape(expert_count, bucket_size, model_width)
    gate_cols = w_gate[0]
    up_cols = w_up[0]
    down_rows = w_down[0]
    arrived = lax.all_to_all(buckets, "expert", split_axis=0, concat_axis=0, tiled=True).reshape(
        -1, model_width
    )
    hidden = expand_rows(
        lax.all_gather(arrived, ("vocab", "batch"), axis=0, tiled=True), gate_cols, up_cols
    )
    expert_sum = lax.psum_scatter(
        jnp.dot(hidden, down_rows, preferred_element_type=jnp.float32).astype(jnp.bfloat16),
        ("vocab", "batch"),
        scatter_dimension=0,
        tiled=True,
    )
    outgoing = expert_sum.reshape(expert_count, bucket_size, model_width)
    returned = lax.all_to_all(outgoing, "expert", split_axis=0, concat_axis=0, tiled=True)
    returned_rows = returned.reshape(-1, model_width).astype(jnp.float32)
    mixed_rows = stream + jnp.dot(combine_weights, returned_rows, precision=lax.Precision.HIGHEST)
    normed_out = rms_scale(mixed_rows, final_gain).astype(jnp.bfloat16)
    head_index = lax.axis_index(("expert", "vocab"))
    vocab_share = lm_head.shape[0]
    vocab_ids = jnp.arange(vocab_share, dtype=jnp.int32) + head_index * vocab_share
    targets = target_ids[0]
    group_tokens = targets.shape[0]
    logits = lax.dot_general(
        lax.all_gather(normed_out, ("expert", "vocab"), axis=0, tiled=True),
        lm_head,
        (((1,), (1,)), ((), ())),
        preferred_element_type=jnp.float32,
    )
    block_top = jnp.max(logits, axis=1)
    block_sum = jnp.sum(jnp.exp(logits - block_top[:, None]), axis=1)
    block_hit = jnp.sum(jnp.where(targets[:, None] == vocab_ids[None, :], logits, 0.0), axis=1)
    fresh = (block_top, block_sum, block_hit)
    largest, spread_sum, chosen = tuple((fresh[slot] for slot in range(3)))
    lengths = choice_len[0]
    questions = choice_question[0]
    own_first = head_index * token_count
    group_positions = jnp.arange(group_tokens, dtype=jnp.int32)
    best, summed, target_sum = joined(
        (largest, spread_sum, chosen), ("expert", "vocab"), merge_stats
    )
    group_logprob = target_sum - (best + jnp.log(summed))
    choice_total = jnp.sum(
        jnp.where(choice_member(lengths, group_positions), group_logprob[None, :], 0.0), axis=1
    )
    own_logprob = lax.dynamic_slice_in_dim(group_logprob, own_first, token_count, 0)
    choice_prob = choice_softmax(choice_total, lengths, questions)
    return (own_logprob.reshape(1, -1), choice_prob.reshape(1, -1))


MESH = pl.DeviceIdType.MESH
VMEM_BYTES = 67043328
CHUNKS = 6


def greet(partners):
    barrier = pltpu.get_barrier_semaphore()
    for partner in partners:
        pl.semaphore_signal(barrier, inc=1, device_id=partner, device_id_type=MESH)
    pl.semaphore_wait(barrier, len(partners))


def push(src, dst, send_sem, recv_sem, partner):
    return pltpu.make_async_remote_copy(
        src_ref=src,
        dst_ref=dst,
        send_sem=send_sem,
        recv_sem=recv_sem,
        device_id=partner,
        device_id_type=MESH,
    )


PAIRS = CHUNKS // 2
FIRST_ORDER = (
    "p0", "p1", "r0", "r1", "p2", "r2", "c0", "r3", "c1", "r4", "e0", "r5", "c2", "e1", "c3", "e2",
    "c4", "e3", "c5", "e4", "e5",
)
SECOND_ORDER = (
    "d0", "d1", "d2", "s0", "d3", "s1", "d4", "s2", "d5", "s3", "a0", "a1", "s4", "s5", "a2", "b0",
    "a3", "b1", "a4", "a5", "b2", "b3", "b4", "b5", "m0", "m1", "f0", "m2", "f1", "f2", "h0", "f3",
    "h1", "f4", "h2", "f5", "h3", "h4", "h5",
)


def row_cap(ne, tokens, routes):
    return max(2, (tokens * routes + ne - 1) // ne + 1)


def wide(value):
    return value.astype(jnp.float32)


def iota(shape, axis):
    return lax.broadcasted_iota(jnp.int32, shape, axis)


def landed(ref, send_sem, recv_sem, partner):
    push(ref, ref, send_sem, recv_sem, partner).wait_recv()


def sent(ref, send_sem, recv_sem, partner):
    push(ref, ref, send_sem, recv_sem, partner).wait_send()


def run(order, stages):
    for word in order:
        with jax.named_scope(word):
            stages[word[0]](int(word[1:]))


def as_column(row, count):
    eye = iota((count, row.shape[1]), 0) == iota((count, row.shape[1]), 1)
    return jnp.sum(jnp.where(eye, row, 0.0), axis=1, keepdims=True)


def as_row(column, lanes):
    count = column.shape[0]
    eye = iota((count, lanes), 0) == iota((count, lanes), 1)
    return jnp.sum(jnp.where(eye, column, 0.0), axis=0, keepdims=True)


def fused_kernel(
    ne,
    nv,
    nb,
    cap,
    resid_any,
    moe_gain_any,
    final_gain_any,
    router_any,
    ids_any,
    target_any,
    length_any,
    question_any,
    wg_hbm,
    wu_hbm,
    wd_hbm,
    head_hbm,
    out_ref,
    resid_ref,
    moe_gain_ref,
    final_gain_ref,
    router_ref,
    ids_ref,
    target_ref,
    length_ref,
    question_ref,
    big,
    wd,
    zout,
    zin,
    xs,
    xl,
    g_acc,
    u_acc,
    hid,
    pm,
    po,
    rpair,
    sy,
    ry,
    sx,
    rx,
    zs,
    zo,
    ys,
    logits,
    scales,
    stats,
    i_sem,
    w_sem,
    wd_sem,
    h_sem,
    z_send,
    z_recv,
    c_send,
    c_recv,
    m_send,
    m_recv,
    r_send,
    r_recv,
    o_send,
    o_recv,
    y_send,
    y_recv,
    x_recv,
    s_send,
    s_recv,
):
    e, v, b = lax.axis_index("expert"), lax.axis_index("vocab"), lax.axis_index("batch")
    core = lax.rem(b, 2)
    other = 1 - core
    tokens, width = resid_ref.shape
    half = width // 2
    n = CHUNKS
    cw = half // n
    pw = 2 * cw
    zw = pw * 5 // 8
    chip_rows = ne * 2 * cap
    tiles = chip_rows // 8
    rows = 4 * chip_rows
    hidden = hid.shape[1]
    share = head_hbm.shape[0]
    block = big.shape[1]
    peers = ne * nv
    me = e * nv + v
    across = (e, 1 - v, b)
    along = (e, v, lax.rem(b + 2, 4))
    turned = b + 1 - 2 * core
    mate = (e, v, turned)
    bf16 = jnp.bfloat16

    def cols(j):
        return pl.ds(j * cw, cw)

    column = []
    for k in range(ne):
        for s in range(2):
            if k + s > 0:
                to = lax.rem(e + k, ne)
                column.append((k * 2 + s, to, other if s else core, (to, v, turned if s else b)))

    def packed(p):
        return pl.ds(p * zw, zw)

    def stacked(value, count):
        part = value.shape[1] // count
        return jnp.concatenate([value[:, g * part : (g + 1) * part] for g in range(count)], axis=0)

    def at(k):
        p = lax.rem(me + k, peers)
        return (p // nv, lax.rem(p, nv), b)

    barrier = pltpu.get_barrier_semaphore()
    greeted = [where for _, _, _, where in column]
    greeted += [(lax.rem(e + k, ne), 1 - v, b) for k in range(ne)] + [along]
    for partner in greeted:
        pl.semaphore_signal(barrier, inc=1, device_id=partner, device_id_type=MESH)

    input_loads = [
        pltpu.make_async_copy(source, target, i_sem.at[i])
        for i, (source, target) in enumerate(
            (
                (resid_any, resid_ref),
                (moe_gain_any, moe_gain_ref),
                (ids_any, ids_ref),
                (router_any, router_ref),
                (final_gain_any, final_gain_ref),
                (target_any, target_ref),
                (length_any, length_ref),
                (question_any, question_ref),
            )
        )
    ]
    for load in input_loads:
        load.start()
    for load in input_loads[:3]:
        load.wait()

    stream = wide(resid_ref[...])
    mean_square = jnp.sum(stream * stream, axis=1, keepdims=True) * (1.0 / width)
    normed = wide((stream * lax.rsqrt(mean_square + epsilon) * moe_gain_ref[...]).astype(bf16))
    ids = wide(ids_ref[...])
    first_row, second_row = ids[0:1, :], ids[1:2, :]
    expert_of = wide(lax.shift_right_logical(iota((ne * 8, tokens), 0), 3))
    line_of = iota((ne * 8, tokens), 0) & 7
    named = (first_row == expert_of) | (second_row == expert_of)
    before = jnp.where(iota((tokens, tokens), 0) < iota((tokens, tokens), 1), 1.0, 0.0)
    rank = jnp.dot(jnp.where(named, 1.0, 0.0), before, preferred_element_type=jnp.float32)
    four = jnp.where(named & (rank == wide(line_of & 3)), 1.0, 0.0)
    fifth = jnp.where(named & (rank == 4.0), 1.0, 0.0)
    pick_four = jnp.concatenate(
        [jnp.where(line_of < 4, four, 0.0), jnp.where(line_of < 4, 0.0, four)], axis=1
    )
    pick_fifth = jnp.concatenate([jnp.where(line_of == g, fifth, 0.0) for g in range(8)], axis=1)

    def product(left, right):
        return jnp.dot(left, right, preferred_element_type=jnp.float32)

    for p in range(PAIRS):
        for h in range(2):
            piece = normed[:, h * half + p * pw : h * half + (p + 1) * pw]
            zout[h, :, :, p * zw : p * zw + cw] = (
                product(pick_four, stacked(piece, 2)).reshape(ne, 8, cw).astype(bf16)
            )
            zout[h, :, :, p * zw + cw : (p + 1) * zw] = (
                product(pick_fifth, stacked(piece, 8)).reshape(ne, 8, zw - cw).astype(bf16)
            )
    pl.semaphore_wait(barrier, len(greeted))

    z_copies = {}
    for p in range(PAIRS):
        for slot, to, ct, where in column:
            z_copies[p, slot] = push(
                zout.at[ct, to, :, packed(p)],
                zin.at[e * 2 + core, :, packed(p)],
                z_send.at[0],
                z_recv.at[p],
                where,
            )
            z_copies[p, slot].start()
    zin[e * 2 + core] = zout[core, e]

    for j in range(n):
        for which, source in enumerate((wg_hbm, wu_hbm)):
            for h in range(2):
                first = h * half + j * cw
                pltpu.make_async_copy(
                    source.at[0, pl.ds(first, cw)],
                    big.at[pl.ds(which * width + first, cw)],
                    w_sem.at[j],
                ).start()
    down_load = pltpu.make_async_copy(wd_hbm.at[0], wd, wd_sem.at[0])
    down_load.start()
    for load in input_loads[3:]:
        load.wait()
    first_id, second_id = as_column(first_row, tokens), as_column(second_row, tokens)
    expert_lane = wide(lax.shift_right_logical(iota((tokens, ne * 8), 1), 3))
    line_lane = iota((tokens, ne * 8), 1) & 7
    first_here, second_here = first_id == expert_lane, second_id == expert_lane
    after = jnp.where(iota((tokens, tokens), 1) < iota((tokens, tokens), 0), 1.0, 0.0)
    rank = jnp.dot(
        after, jnp.where(first_here | second_here, 1.0, 0.0), preferred_element_type=jnp.float32
    )
    first_logit = jnp.zeros((tokens, 1), jnp.float32)
    second_logit = jnp.zeros((tokens, 1), jnp.float32)
    for k in range(ne):
        router_logit = jnp.sum(normed * wide(router_ref[k : k + 1, :]), axis=1, keepdims=True)
        first_logit = first_logit + jnp.where(first_id == k, router_logit, 0.0)
        second_logit = second_logit + jnp.where(second_id == k, router_logit, 0.0)
    first_gate = 1.0 / (1.0 + jnp.exp(second_logit - first_logit))
    second_gate = 1.0 / (1.0 + jnp.exp(first_logit - second_logit))
    gate = jnp.where(first_here, first_gate, jnp.where(second_here, second_gate, 0.0))
    four = jnp.where(rank == wide(line_lane & 3), gate, 0.0)
    fifth = jnp.where(rank == 4.0, gate, 0.0)

    def two_terms(weights):
        weights = jnp.concatenate(weights, axis=0)
        coarse = wide(weights.astype(bf16))
        return jnp.concatenate([coarse, weights - coarse], axis=0).astype(bf16)

    mix_four = two_terms([jnp.where(line_lane < 4, four, 0.0), jnp.where(line_lane < 4, 0.0, four)])
    mix_fifth = two_terms([jnp.where(line_lane == g, fifth, 0.0) for g in range(8)])

    sources = 2 * ne
    moved = (sources * 8, sources * 8)

    def four_place(axis):
        index = iota(moved, axis)
        side = jnp.where(index < sources * 4, 0, 1)
        within = index - side * (sources * 4)
        target = lax.shift_right_logical(within, 2) * 8 + side * 4 + (within & 3)
        return jnp.where(target == iota(moved, 1 - axis), 1.0, 0.0).astype(bf16)

    def fifth_place(axis):
        index, target = iota(moved, axis), iota(moved, 1 - axis)
        fits = ((target & 7) * sources + lax.shift_right_logical(target, 3)) == index
        return jnp.where(fits, 1.0, 0.0).astype(bf16)

    open_four, open_fifth = four_place(0), fifth_place(0)
    close_four, close_fifth = four_place(1), fifth_place(1)

    def plane_push(src_slot, dst_slot, j, partner):
        return push(
            xs.at[src_slot, core, :, :, cols(j)],
            xs.at[dst_slot, core, :, :, cols(j)],
            c_send.at[0],
            c_recv.at[j, dst_slot - 1],
            partner,
        )

    c_copies, m_copies = {}, {}

    def mate_push(slot, j):
        m_copies[j, slot] = push(
            xs.at[slot, core, :, :, cols(j)],
            xs.at[slot, core, :, :, cols(j)],
            m_send.at[0],
            m_recv.at[j],
            mate,
        )
        m_copies[j, slot].start()

    def open_pair(p):
        landed(zin.at[: sources - 1, :, packed(p)], z_send.at[0], z_recv.at[p], mate)
        block_rows = wide(zin[:, :, packed(p)])
        fours = product(
            open_four, block_rows[:, :, :cw].reshape(sources * 8, cw).astype(bf16)
        ).reshape(2, ne, 8, cw)
        fifths = product(
            open_fifth, block_rows[:, :, cw:].reshape(sources * 8, zw - cw).astype(bf16)
        )
        for side in range(2):
            j = 2 * p + side
            xs[0, core, 0:ne, :, cols(j)] = fours[side].astype(bf16)
            row = [
                fifths[g * sources : (g + 1) * sources] for g in range(side * 4, side * 4 + 4)
            ]
            xs[0, core, ne, :, cols(j)] = jnp.concatenate(row, axis=1).astype(bf16)
            for slot, partner in ((1, across), (2, along)):
                c_copies[j, slot] = plane_push(0, slot, j, partner)
                c_copies[j, slot].start()
            mate_push(0, j)

    def relay(j):
        source, partner = (1, along) if j % 2 == 0 else (2, across)
        c_copies[j, source].wait_recv()
        c_copies[j, 3] = plane_push(source, 3, j, partner)
        c_copies[j, 3].start()
        mate_push(source, j)
        c_copies[j, 3 - source].wait_recv()
        mate_push(3 - source, j)

    def corner(j):
        c_copies[j, 3].wait_recv()
        mate_push(3, j)

    tile = min(256, hidden)

    def expand(j):
        landed(xs.at[:, other, :, :, cols(j)], m_send.at[0], m_recv.at[j], mate)
        for h in range(2):
            xl[h] = wide(xs[:, h, :, :, cols(j)]).reshape(rows, cw).astype(bf16)
        pltpu.make_async_copy(
            head_hbm.at[pl.ds(0, 4 * cw), pl.ds(0, hidden)], big.at[pl.ds(0, 4 * cw)], w_sem.at[j]
        ).wait()

        for i in range(hidden // tile):
            where = pl.ds(i * tile, tile)

            def raw(which):
                low = which * width + j * cw
                return product(xl[0], big[low : low + cw, where]) + product(
                    xl[1], big[low + half : low + half + cw, where]
                )

            g, u = raw(0), raw(1)
            if j > 0:
                g, u = g + g_acc[:, where], u + u_acc[:, where]
            if j < n - 1:
                g_acc[:, where] = g
                u_acc[:, where] = u
            else:
                hid[:, where] = (g / (1.0 + jnp.exp(-g)) * u).astype(bf16)

    run(FIRST_ORDER, {"p": open_pair, "r": relay, "c": corner, "e": expand})

    head_loads = []
    per_half = half // block
    for q in range(per_half):
        for h in range(2):
            place = h * per_half + q
            head_loads.append(
                pltpu.make_async_copy(
                    head_hbm.at[:, pl.ds(place * block, block)],
                    big.at[pl.ds(place * share, share)],
                    h_sem.at[place],
                )
            )
            head_loads[-1].start()
    down_load.wait()

    rp, yc, xc, zc, gz, gx = {}, {}, {}, {}, {}, {}

    def down(j):
        def part(side):
            where = pl.ds(pl.multiple_of(side * half + j * cw, 128), cw)
            return product(hid[...], wd[:, where])

        pm[:, :, :, cols(j)] = part(other).reshape(4, tiles, 8, cw).astype(bf16)
        rp[j] = push(
            pm.at[:, :, :, cols(j)], rpair.at[:, :, :, cols(j)], r_send.at[0], r_recv.at[j, 0], mate
        )
        rp[j].start()
        po[:, :, cols(j)] = part(core).reshape(4, chip_rows, cw)

    def pair_sum(j):
        rp[j].wait_recv()
        total = po[:, :, cols(j)] + wide(rpair[:, :, :, cols(j)]).reshape(4, chip_rows, cw)
        kept, passed, partner = ((0, 1), (2, 3), along) if j % 2 == 0 else ((0, 2), (1, 3), across)
        for i in range(2):
            sy[i, :, :, cols(j)] = total[passed[i]].reshape(tiles, 8, cw).astype(bf16)
        yc[j] = push(
            sy.at[:, :, :, cols(j)], ry.at[:, :, :, cols(j)], r_send.at[1], r_recv.at[j, 1], partner
        )
        yc[j].start()
        for i in range(2):
            po[i, :, cols(j)] = total[kept[i]]

    def side_sum(j):
        yc[j].wait_recv()
        total = po[1, :, cols(j)] + wide(ry[1, :, :, cols(j)]).reshape(chip_rows, cw)
        sx[:, :, cols(j)] = total.reshape(tiles, 8, cw).astype(bf16)
        partner = across if j % 2 == 0 else along
        xc[j] = push(
            sx.at[:, :, cols(j)], rx.at[:, :, cols(j)], r_send.at[2], r_recv.at[j, 2], partner
        )
        xc[j].start()
        po[0, :, cols(j)] = po[0, :, cols(j)] + wide(ry[0, :, :, cols(j)]).reshape(chip_rows, cw)

    def own_sum(j):
        xc[j].wait_recv()
        po[0, :, cols(j)] = po[0, :, cols(j)] + wide(rx[:, :, cols(j)]).reshape(chip_rows, cw)
        if j % 2 == 0:
            return
        p = j // 2
        total = po[0, :, p * pw : (p + 1) * pw]
        fours = product(close_four, stacked(total[: sources * 4], 2).astype(bf16))
        fifths = product(close_fifth, stacked(total[sources * 4 :], 8).astype(bf16))
        zs[:, :, :, p * zw : p * zw + cw] = fours.reshape(ne, 2, 8, cw).astype(bf16)
        zs[:, :, :, p * zw + cw : (p + 1) * zw] = fifths.reshape(ne, 2, 8, zw - cw).astype(bf16)
        for slot, to, ct, where in column:
            zc[p, slot] = push(
                zs.at[to, ct, :, packed(p)],
                zo.at[e * 2 + core, :, packed(p)],
                o_send.at[0],
                o_recv.at[p],
                where,
            )
            zc[p, slot].start()
        zo[e * 2 + core, :, packed(p)] = zs[e, core, :, packed(p)]

    squares = [jnp.zeros((tokens, 1), jnp.float32)]

    def mix(p):
        landed(zo.at[: sources - 1, :, packed(p)], o_send.at[0], o_recv.at[p], mate)
        every = wide(zo[:, :, packed(p)]).reshape(ne, 2, 8, zw)
        for h in range(2):
            fours = product(mix_four, every[:, h, :, :cw].reshape(ne * 8, cw).astype(bf16))
            fours = fours[: 2 * tokens] + fours[2 * tokens :]
            fifths = product(mix_fifth, every[:, h, :, cw:].reshape(ne * 8, zw - cw).astype(bf16))
            fifths = fifths[: 8 * tokens] + fifths[8 * tokens :]
            for side in range(2):
                j = 2 * p + side
                first = h * half + j * cw
                row = [fifths[g * tokens : (g + 1) * tokens] for g in range(side * 4, side * 4 + 4)]
                weighted = fours[side * tokens : (side + 1) * tokens] + jnp.concatenate(row, axis=1)
                mixed = wide(resid_ref[:, first : first + cw]) + weighted
                squares[0] = squares[0] + jnp.sum(mixed * mixed, axis=1, keepdims=True)
                ys[me, j, h] = (mixed * final_gain_ref[:, first : first + cw]).astype(bf16)
        for j in (2 * p, 2 * p + 1):
            for k in range(1, ne):
                gz[j, k] = push(
                    ys.at[me, j],
                    ys.at[me, j],
                    y_send.at[0],
                    y_recv.at[j, k - 1],
                    (lax.rem(e + k, ne), v, b),
                )
                gz[j, k].start()
            turn(j, 0)
        if p == PAIRS - 1:
            share_scale()

    def turn(j, k):
        slot = lax.rem(e + ne - k, ne) * nv + v
        gx[j, k] = push(
            ys.at[slot, j], ys.at[slot, j], y_send.at[1], x_recv.at[j], across
        )
        gx[j, k].start()

    def forward(j):
        for k in (1, 3, 2):
            gz[j, k].wait_recv()
            turn(j, k)

    head_tile = min(256, share)

    def head(j):
        landed(ys.at[:ne, j], y_send.at[1], x_recv.at[j], across)
        if (j * cw) % block == 0:
            for h in range(2):
                head_loads[(j * cw) // block * 2 + h].wait()
        sides = []
        for h in range(2):
            sides.append(wide(ys[:, j, h]).reshape(peers * tokens, cw).astype(bf16))
        left = (j * cw) % block
        low = (j * cw) // block * share

        for i in range(share // head_tile):
            first = i * head_tile
            found = 0.0
            for h in range(2):
                found = found + lax.dot_general(
                    sides[h],
                    big[pl.ds(low + h * per_half * share + first, head_tile), left : left + cw],
                    (((1,), (1,)), ((), ())),
                    preferred_element_type=jnp.float32,
                )
            if j > 0:
                found = found + logits[:, pl.ds(first, head_tile)]
            logits[:, pl.ds(first, head_tile)] = found

    small = []

    def share_scale():
        scale = lax.rsqrt(squares[0] * (1.0 / width) + epsilon)
        scales[me] = jnp.broadcast_to(scale, (tokens, 128))
        for k in range(1, peers):
            small.append(
                push(scales.at[me], scales.at[me], s_send.at[0], s_recv.at[0], at(k))
            )
            small[-1].start()

    run(
        SECOND_ORDER,
        {
            "d": down,
            "s": pair_sum,
            "a": side_sum,
            "b": own_sum,
            "m": mix,
            "f": forward,
            "h": head,
        },
    )

    landed(scales.at[: peers - 1], s_send.at[0], s_recv.at[0], mate)
    group = peers * tokens
    lanes = 128
    scaled = logits[...] * scales[...].reshape(group, lanes)[:, 0:1]
    targets = as_column(wide(target_ref[...]), group)
    vocab_ids = wide(iota((group, share), 1) + me * share)
    top = jnp.max(scaled, axis=1, keepdims=True)
    total = jnp.sum(jnp.exp(scaled - top), axis=1, keepdims=True)
    hit = jnp.sum(jnp.where(vocab_ids == targets, scaled, 0.0), axis=1, keepdims=True)
    line = iota((8, lanes), 0)
    stats[me] = jnp.where(
        line == 0,
        as_row(top, lanes),
        jnp.where(line == 1, as_row(total, lanes), jnp.where(line == 2, as_row(hit, lanes), 0.0)),
    )
    sends = [
        push(stats.at[me], stats.at[me], s_send.at[1], s_recv.at[1], at(k))
        for k in range(1, peers)
    ]
    for copy in sends:
        copy.start()

    choices = length_ref.shape[1]
    lengths_row, questions_row = wide(length_ref[...]), wide(question_ref[...])
    lengths, questions = as_column(lengths_row, choices), as_column(questions_row, choices)
    square = (choices, choices)
    ends = jnp.sum(jnp.where(iota(square, 1) <= iota(square, 0), lengths_row, 0.0), axis=1, keepdims=True)
    place = wide(iota((choices, lanes), 1))
    member = (place >= ends - lengths) & (place < ends)
    same = questions == questions_row

    landed(stats.at[: peers - 1], s_send.at[1], s_recv.at[1], mate)
    every = stats[...]
    best = jnp.max(every[:, 0:1, :], axis=0)
    summed = jnp.sum(every[:, 1:2, :] * jnp.exp(every[:, 0:1, :] - best[None]), axis=0)
    chosen = jnp.sum(every[:, 2:3, :], axis=0)
    used = iota((1, lanes), 1) < group
    logprob = jnp.where(used, chosen - (best + jnp.log(jnp.where(used, summed, 1.0))), 0.0)
    own = jnp.sum(
        jnp.where(iota((tokens, lanes), 1) == iota((tokens, lanes), 0) + me * tokens, logprob, 0.0),
        axis=1,
        keepdims=True,
    )
    found = as_row(own, lanes)
    average = jnp.sum(jnp.where(member, logprob, 0.0), axis=1, keepdims=True) / lengths
    question_top = jnp.max(
        jnp.where(same, as_row(average, choices), -jnp.inf), axis=1, keepdims=True
    )
    raised = jnp.exp(average - question_top)
    denominator = jnp.sum(jnp.where(same, as_row(raised, choices), 0.0), axis=1, keepdims=True)
    prob = raised / denominator
    far = iota((choices, lanes), 1) == iota((choices, lanes), 0) + tokens
    out_ref[...] = found + jnp.sum(jnp.where(far, prob, 0.0), axis=0, keepdims=True)

    for ref, send, recv in (
        (zin.at[: 2 * ne - 1], z_send.at[0], z_recv.at[0]),
        (xs.at[:3, 0], c_send.at[0], c_recv.at[0, 0]),
        (xs.at[:, 0], m_send.at[0], m_recv.at[0]),
        (pm, r_send.at[0], r_recv.at[0, 0]),
        (sy, r_send.at[1], r_recv.at[0, 1]),
        (sx, r_send.at[2], r_recv.at[0, 2]),
        (zo.at[: 2 * ne - 1], o_send.at[0], o_recv.at[0]),
        (ys.at[: ne - 1], y_send.at[0], y_recv.at[0, 0]),
        (ys.at[:ne], y_send.at[1], x_recv.at[0]),
        (scales.at[: peers - 1], s_send.at[0], s_recv.at[0]),
        (stats.at[: peers - 1], s_send.at[1], s_recv.at[1]),
    ):
        sent(ref, send, recv, mate)


def fused_call(sizes, resid, moe_gain, final_gain, router, ids, targets, lengths, questions, *weights):
    ne, nv, nb = sizes
    tokens, width = resid.shape
    w_gate, _, _, lm_head = weights
    hidden = w_gate.shape[2]
    share = lm_head.shape[0]
    cap = row_cap(ne, tokens, ids.shape[0])
    half = width // 2
    tiles = ne * 2 * cap // 8
    rows = 4 * tiles * 8
    peers = ne * nv
    n = CHUNKS
    cw = half // n
    zw = half * 5 // 8
    bf16, f32 = jnp.bfloat16, jnp.float32
    dma = pltpu.SemaphoreType.DMA
    vmem = pltpu.VMEM
    vm = pl.BlockSpec(memory_space=pltpu.VMEM)
    anywhere = pl.BlockSpec(memory_space=pl.ANY)
    return pl.pallas_call(
        functools.partial(fused_kernel, ne, nv, nb, cap),
        out_shape=pltpu.VMEM((1, 128), f32),
        in_specs=[anywhere] * 12,
        out_specs=vm,
        scratch_shapes=[
            vmem(resid.shape, bf16),
            vmem(moe_gain.shape, f32),
            vmem(final_gain.shape, f32),
            vmem(router.shape, bf16),
            vmem(ids.shape, jnp.int32),
            vmem(targets.shape, jnp.int32),
            vmem(lengths.shape, jnp.int32),
            vmem(questions.shape, jnp.int32),
            vmem((2 * width, hidden), bf16),
            vmem((hidden, width), bf16),
            vmem((2, ne, 8, zw), bf16),
            vmem((2 * ne, 8, zw), bf16),
            vmem((4, 2, tiles, 8, half), bf16),
            vmem((2, rows, cw), bf16),
            vmem((rows, hidden), f32),
            vmem((rows, hidden), f32),
            vmem((rows, hidden), bf16),
            vmem((4, tiles, 8, half), bf16),
            vmem((4, tiles * 8, half), f32),
            vmem((4, tiles, 8, half), bf16),
            vmem((2, tiles, 8, half), bf16),
            vmem((2, tiles, 8, half), bf16),
            vmem((tiles, 8, half), bf16),
            vmem((tiles, 8, half), bf16),
            vmem((ne, 2, 8, zw), bf16),
            vmem((2 * ne, 8, zw), bf16),
            vmem((peers, n, 2, 8, cw), bf16),
            vmem((peers * tokens, share), f32),
            vmem((peers, tokens, 128), f32),
            vmem((peers, 8, 128), f32),
            dma((8,)),
            dma((n,)),
            dma((1,)),
            dma((width // hidden,)),
            dma((1,)),
            dma((PAIRS,)),
            dma((1,)),
            dma((n, 3)),
            dma((1,)),
            dma((n,)),
            dma((3,)),
            dma((n, 3)),
            dma((1,)),
            dma((PAIRS,)),
            dma((2,)),
            dma((n, 3)),
            dma((n,)),
            dma((2,)),
            dma((2,)),
        ],
        compiler_params=pltpu.CompilerParams(
            collective_id=0, has_side_effects=True, vmem_limit_bytes=VMEM_BYTES - 1024 * 1024
        ),
        name="fused",
    )(resid, moe_gain, final_gain, router, ids, targets, lengths, questions, *weights)


def kernel_fits(sizes, *arrays):
    ne, nv, nb = sizes
    resid, w_gate, lm_head, ids = arrays[0], arrays[4], arrays[7], arrays[8]
    tokens, width = resid.shape[1:]
    hidden = w_gate.shape[2]
    share = lm_head.shape[0]
    cap = row_cap(ne, tokens, ids.shape[2])
    rows = 8 * ne * cap
    need = 2 * (3 * width * hidden + rows * (4 * width + 6 * hidden) + 8 * ne * 8 * width)
    return (
        ne == 4
        and nv == 2
        and nb == 4
        and tokens == 8
        and ids.shape[2] == 2
        and cap == 5
        and ne * 2 * cap % 8 == 0
        and width % (2 * hidden) == 0
        and width % (2 * CHUNKS * 512) == 0
        and hidden % (width // 2 // CHUNKS) == 0
        and hidden % 256 == 0
        and share == 2 * hidden
        and ne * nv * tokens <= 128
        and need < VMEM_BYTES - 4 * 1024 * 1024
    )


def on_device_kernel(
    sizes,
    resid,
    moe_gain,
    final_gain,
    router,
    w_gate,
    w_up,
    w_down,
    lm_head,
    expert_ids,
    target_ids,
    choice_len,
    choice_question,
):
    found = fused_call(
        sizes,
        resid[0],
        moe_gain.reshape(1, -1),
        final_gain.reshape(1, -1),
        router.T,
        expert_ids[0].T,
        target_ids,
        choice_len,
        choice_question,
        w_gate,
        w_up,
        w_down,
        lm_head,
    )
    tokens = resid.shape[1]
    return found[:, :tokens], found[:, tokens : tokens + choice_len.shape[1]]


def either(sizes, *arrays):
    if kernel_fits(sizes, *arrays):
        return on_device_kernel(sizes, *arrays)
    return on_device(*arrays)


def solution(mesh):
    sizes = tuple(mesh.shape[axis] for axis in ("expert", "vocab", "batch"))
    return jax.shard_map(
        functools.partial(either, sizes),
        mesh=mesh,
        in_specs=(
            P("batch", ("expert", "vocab"), None),
            P(),
            P(),
            P(),
            P("expert", None, ("vocab", "batch")),
            P("expert", None, ("vocab", "batch")),
            P("expert", ("vocab", "batch"), None),
            P(("expert", "vocab"), None),
            P("batch", ("expert", "vocab"), None),
            P("batch", None),
            P("batch", None),
            P("batch", None),
        ),
        out_specs=(P("batch", ("expert", "vocab")), P("batch", None)),
        check_vma=False,
    )
```

```python
import functools

import jax
import jax.numpy as jnp
from jax import lax
from jax.experimental import pallas as pl
from jax.experimental.pallas import tpu as pltpu
from jax.sharding import PartitionSpec as P

epsilon = 1e-05


def joined(array, axis, combine):
    everything = jax.tree.map(lambda part: lax.all_gather(part, axis), array)
    leading = jax.tree.map(lambda part: part[0], everything)

    def lap(k, so_far):
        return combine(so_far, jax.tree.map(lambda part: part[k], everything))

    return lax.fori_loop(1, lax.axis_size(axis), lap, leading)


def rms_scale(values, gain):
    mean_square = jnp.mean(values * values, axis=-1, keepdims=True)
    return values * lax.rsqrt(mean_square + epsilon) * gain


def route_gates(router_logit, route_ids):
    expert_count = router_logit.shape[1]
    matches = route_ids[:, :, None] == jnp.arange(expert_count, dtype=jnp.int32)[None, None, :]
    picked = jnp.sum(jnp.where(matches, router_logit[:, None, :], 0.0), axis=2)
    return 1.0 / jnp.sum(jnp.exp(picked[:, None, :] - picked[:, :, None]), axis=2)


def expand_rows(block_rows, gate_cols, up_cols):
    gate_part = jnp.dot(block_rows, gate_cols, preferred_element_type=jnp.float32)
    up_part = jnp.dot(block_rows, up_cols, preferred_element_type=jnp.float32)
    return (jax.nn.silu(gate_part) * up_part).astype(jnp.bfloat16)


def choice_member(lengths, positions):
    ends = jnp.cumsum(lengths, dtype=jnp.int32)
    starts = ends - lengths
    return (positions[None, :] >= starts[:, None]) & (positions[None, :] < ends[:, None])


def choice_softmax(choice_total, lengths, questions):
    average = choice_total / lengths.astype(jnp.float32)
    same_question = questions[:, None] == questions[None, :]
    question_top = jnp.max(jnp.where(same_question, average[None, :], -jnp.inf), axis=1)
    raised = jnp.exp(average - question_top)
    denominator = jnp.sum(jnp.where(same_question, raised[None, :], 0.0), axis=1)
    return raised / denominator


def merge_stats(first, second):
    top_value = jnp.maximum(first[0], second[0])
    summed = first[1] * jnp.exp(first[0] - top_value) + second[1] * jnp.exp(second[0] - top_value)
    return (top_value, summed, first[2] + second[2])


def on_device(
    resid,
    moe_gain,
    final_gain,
    router,
    w_gate,
    w_up,
    w_down,
    lm_head,
    expert_ids,
    target_ids,
    choice_len,
    choice_question,
):
    stream = resid[0].astype(jnp.float32)
    token_count, model_width = stream.shape
    normed_in = rms_scale(stream, moe_gain).astype(jnp.bfloat16)
    router_logit = jnp.dot(normed_in, router, preferred_element_type=jnp.float32)
    route_ids = expert_ids[0]
    route_count = route_ids.shape[1]
    gate_weights = route_gates(router_logit, route_ids)
    expert_count = lax.axis_size("expert")
    bucket_size = max(2, (token_count * route_count + expert_count - 1) // expert_count + 1)
    flat_ids = route_ids.reshape(-1)
    expert_match = (flat_ids[:, None] == jnp.arange(expert_count, dtype=jnp.int32)[None, :]).astype(
        jnp.int32
    )
    earlier = jnp.cumsum(expert_match, axis=0, dtype=jnp.int32) - expert_match
    slot_index = flat_ids * bucket_size + jnp.sum(earlier * expert_match, axis=1)
    slot_match = (
        slot_index[:, None] == jnp.arange(expert_count * bucket_size, dtype=jnp.int32)[None, :]
    ).astype(jnp.float32)
    slot_match = slot_match.reshape(token_count, route_count, -1)
    dispatch = jnp.sum(slot_match, axis=1).astype(jnp.bfloat16)
    combine_weights = jnp.sum(slot_match * gate_weights[:, :, None], axis=1)
    buckets = lax.dot_general(
        dispatch, normed_in, (((0,), (0,)), ((), ())), preferred_element_type=jnp.float32
    )
    buckets = buckets.astype(jnp.bfloat16).reshape(expert_count, bucket_size, model_width)
    gate_cols = w_gate[0]
    up_cols = w_up[0]
    down_rows = w_down[0]
    arrived = lax.all_to_all(buckets, "expert", split_axis=0, concat_axis=0, tiled=True).reshape(
        -1, model_width
    )
    hidden = expand_rows(
        lax.all_gather(arrived, ("vocab", "batch"), axis=0, tiled=True), gate_cols, up_cols
    )
    expert_sum = lax.psum_scatter(
        jnp.dot(hidden, down_rows, preferred_element_type=jnp.float32).astype(jnp.bfloat16),
        ("vocab", "batch"),
        scatter_dimension=0,
        tiled=True,
    )
    outgoing = expert_sum.reshape(expert_count, bucket_size, model_width)
    returned = lax.all_to_all(outgoing, "expert", split_axis=0, concat_axis=0, tiled=True)
    returned_rows = returned.reshape(-1, model_width).astype(jnp.float32)
    mixed_rows = stream + jnp.dot(combine_weights, returned_rows, precision=lax.Precision.HIGHEST)
    normed_out = rms_scale(mixed_rows, final_gain).astype(jnp.bfloat16)
    head_index = lax.axis_index(("expert", "vocab"))
    vocab_share = lm_head.shape[0]
    vocab_ids = jnp.arange(vocab_share, dtype=jnp.int32) + head_index * vocab_share
    targets = target_ids[0]
    group_tokens = targets.shape[0]
    logits = lax.dot_general(
        lax.all_gather(normed_out, ("expert", "vocab"), axis=0, tiled=True),
        lm_head,
        (((1,), (1,)), ((), ())),
        preferred_element_type=jnp.float32,
    )
    block_top = jnp.max(logits, axis=1)
    block_sum = jnp.sum(jnp.exp(logits - block_top[:, None]), axis=1)
    block_hit = jnp.sum(jnp.where(targets[:, None] == vocab_ids[None, :], logits, 0.0), axis=1)
    fresh = (block_top, block_sum, block_hit)
    largest, spread_sum, chosen = tuple((fresh[slot] for slot in range(3)))
    lengths = choice_len[0]
    questions = choice_question[0]
    own_first = head_index * token_count
    group_positions = jnp.arange(group_tokens, dtype=jnp.int32)
    best, summed, target_sum = joined(
        (largest, spread_sum, chosen), ("expert", "vocab"), merge_stats
    )
    group_logprob = target_sum - (best + jnp.log(summed))
    choice_total = jnp.sum(
        jnp.where(choice_member(lengths, group_positions), group_logprob[None, :], 0.0), axis=1
    )
    own_logprob = lax.dynamic_slice_in_dim(group_logprob, own_first, token_count, 0)
    choice_prob = choice_softmax(choice_total, lengths, questions)
    return (own_logprob.reshape(1, -1), choice_prob.reshape(1, -1))


MESH = pl.DeviceIdType.MESH
VMEM_BYTES = 67043328
CHUNKS = 6


def greet(partners):
    barrier = pltpu.get_barrier_semaphore()
    for partner in partners:
        pl.semaphore_signal(barrier, inc=1, device_id=partner, device_id_type=MESH)
    pl.semaphore_wait(barrier, len(partners))


def push(src, dst, send_sem, recv_sem, partner):
    return pltpu.make_async_remote_copy(
        src_ref=src,
        dst_ref=dst,
        send_sem=send_sem,
        recv_sem=recv_sem,
        device_id=partner,
        device_id_type=MESH,
    )


PAIRS = CHUNKS // 2
FIRST_ORDER = (
    "p0", "p1", "r0", "r1", "p2", "r2", "c0", "r3", "c1", "r4", "e0", "r5", "c2", "e1", "c3", "e2",
    "c4", "e3", "c5", "e4", "e5",
)
SECOND_ORDER = (
    "d0", "d1", "d2", "s0", "d3", "s1", "d4", "s2", "d5", "s3", "a0", "a1", "s4", "s5", "a2", "b0",
    "a3", "b1", "a4", "a5", "b2", "b3", "b4", "b5", "m0", "m1", "f0", "m2", "f1", "f2", "h0", "f3",
    "h1", "f4", "h2", "f5", "h3", "h4", "h5",
)


def row_cap(ne, tokens, routes):
    return max(2, (tokens * routes + ne - 1) // ne + 1)


def wide(value):
    return value.astype(jnp.float32)


def iota(shape, axis):
    return lax.broadcasted_iota(jnp.int32, shape, axis)


def landed(ref, send_sem, recv_sem, partner):
    push(ref, ref, send_sem, recv_sem, partner).wait_recv()


def sent(ref, send_sem, recv_sem, partner):
    push(ref, ref, send_sem, recv_sem, partner).wait_send()


def run(order, stages):
    for word in order:
        with jax.named_scope(word):
            stages[word[0]](int(word[1:]))


def as_column(row, count):
    eye = iota((count, row.shape[1]), 0) == iota((count, row.shape[1]), 1)
    return jnp.sum(jnp.where(eye, row, 0.0), axis=1, keepdims=True)


def as_row(column, lanes):
    count = column.shape[0]
    eye = iota((count, lanes), 0) == iota((count, lanes), 1)
    return jnp.sum(jnp.where(eye, column, 0.0), axis=0, keepdims=True)


def fused_kernel(
    ne,
    nv,
    nb,
    cap,
    resid_any,
    moe_gain_any,
    final_gain_any,
    router_any,
    ids_any,
    target_any,
    length_any,
    question_any,
    wg_hbm,
    wu_hbm,
    wd_hbm,
    head_hbm,
    out_ref,
    resid_ref,
    moe_gain_ref,
    final_gain_ref,
    router_ref,
    ids_ref,
    target_ref,
    length_ref,
    question_ref,
    big,
    wd,
    zout,
    zin,
    xs,
    xl,
    g_acc,
    u_acc,
    hid,
    pm,
    po,
    rpair,
    sy,
    ry,
    sx,
    rx,
    zs,
    zo,
    ys,
    logits,
    scales,
    stats,
    i_sem,
    w_sem,
    wd_sem,
    h_sem,
    z_send,
    z_recv,
    c_send,
    c_recv,
    m_send,
    m_recv,
    r_send,
    r_recv,
    o_send,
    o_recv,
    y_send,
    y_recv,
    x_recv,
    s_send,
    s_recv,
):
    e, v, b = lax.axis_index("expert"), lax.axis_index("vocab"), lax.axis_index("batch")
    core = lax.rem(b, 2)
    other = 1 - core
    tokens, width = resid_ref.shape
    half = width // 2
    n = CHUNKS
    cw = half // n
    pw = 2 * cw
    zw = pw * 5 // 8
    chip_rows = ne * 2 * cap
    tiles = chip_rows // 8
    rows = 4 * chip_rows
    hidden = hid.shape[1]
    share = head_hbm.shape[0]
    block = big.shape[1]
    peers = ne * nv
    me = e * nv + v
    across = (e, 1 - v, b)
    along = (e, v, lax.rem(b + 2, 4))
    turned = b + 1 - 2 * core
    mate = (e, v, turned)
    bf16 = jnp.bfloat16

    def cols(j):
        return pl.ds(j * cw, cw)

    column = []
    for k in range(ne):
        for s in range(2):
            if k + s > 0:
                to = lax.rem(e + k, ne)
                column.append((k * 2 + s, to, other if s else core, (to, v, turned if s else b)))

    def packed(p):
        return pl.ds(p * zw, zw)

    def stacked(value, count):
        part = value.shape[1] // count
        return jnp.concatenate([value[:, g * part : (g + 1) * part] for g in range(count)], axis=0)

    def at(k):
        p = lax.rem(me + k, peers)
        return (p // nv, lax.rem(p, nv), b)

    barrier = pltpu.get_barrier_semaphore()
    greeted = [where for _, _, _, where in column]
    greeted += [(lax.rem(e + k, ne), 1 - v, b) for k in range(ne)] + [along]
    for partner in greeted:
        pl.semaphore_signal(barrier, inc=1, device_id=partner, device_id_type=MESH)

    input_loads = [
        pltpu.make_async_copy(source, target, i_sem.at[i])
        for i, (source, target) in enumerate(
            (
                (resid_any, resid_ref),
                (moe_gain_any, moe_gain_ref),
                (ids_any, ids_ref),
                (router_any, router_ref),
                (final_gain_any, final_gain_ref),
                (target_any, target_ref),
                (length_any, length_ref),
                (question_any, question_ref),
            )
        )
    ]
    for load in input_loads:
        load.start()
    for load in input_loads[:3]:
        load.wait()

    stream = wide(resid_ref[...])
    mean_square = jnp.sum(stream * stream, axis=1, keepdims=True) * (1.0 / width)
    normed = wide((stream * lax.rsqrt(mean_square + epsilon) * moe_gain_ref[...]).astype(bf16))
    ids = wide(ids_ref[...])
    first_row, second_row = ids[0:1, :], ids[1:2, :]
    expert_of = wide(lax.shift_right_logical(iota((ne * 8, tokens), 0), 3))
    line_of = iota((ne * 8, tokens), 0) & 7
    named = (first_row == expert_of) | (second_row == expert_of)
    before = jnp.where(iota((tokens, tokens), 0) < iota((tokens, tokens), 1), 1.0, 0.0)
    rank = jnp.dot(jnp.where(named, 1.0, 0.0), before, preferred_element_type=jnp.float32)
    four = jnp.where(named & (rank == wide(line_of & 3)), 1.0, 0.0)
    fifth = jnp.where(named & (rank == 4.0), 1.0, 0.0)
    pick_four = jnp.concatenate(
        [jnp.where(line_of < 4, four, 0.0), jnp.where(line_of < 4, 0.0, four)], axis=1
    )
    pick_fifth = jnp.concatenate([jnp.where(line_of == g, fifth, 0.0) for g in range(8)], axis=1)

    def product(left, right):
        return jnp.dot(left, right, preferred_element_type=jnp.float32)

    for p in range(PAIRS):
        for h in range(2):
            piece = normed[:, h * half + p * pw : h * half + (p + 1) * pw]
            zout[h, :, :, p * zw : p * zw + cw] = (
                product(pick_four, stacked(piece, 2)).reshape(ne, 8, cw).astype(bf16)
            )
            zout[h, :, :, p * zw + cw : (p + 1) * zw] = (
                product(pick_fifth, stacked(piece, 8)).reshape(ne, 8, zw - cw).astype(bf16)
            )
    pl.semaphore_wait(barrier, len(greeted))

    z_copies = {}
    for p in range(PAIRS):
        for slot, to, ct, where in column:
            z_copies[p, slot] = push(
                zout.at[ct, to, :, packed(p)],
                zin.at[e * 2 + core, :, packed(p)],
                z_send.at[0],
                z_recv.at[p],
                where,
            )
            z_copies[p, slot].start()
    zin[e * 2 + core] = zout[core, e]

    for j in range(n):
        for which, source in enumerate((wg_hbm, wu_hbm)):
            for h in range(2):
                first = h * half + j * cw
                pltpu.make_async_copy(
                    source.at[0, pl.ds(first, cw)],
                    big.at[pl.ds(which * width + first, cw)],
                    w_sem.at[j],
                ).start()
    down_load = pltpu.make_async_copy(wd_hbm.at[0], wd, wd_sem.at[0])
    down_load.start()
    for load in input_loads[3:]:
        load.wait()
    first_id, second_id = as_column(first_row, tokens), as_column(second_row, tokens)
    expert_lane = wide(lax.shift_right_logical(iota((tokens, ne * 8), 1), 3))
    line_lane = iota((tokens, ne * 8), 1) & 7
    first_here, second_here = first_id == expert_lane, second_id == expert_lane
    after = jnp.where(iota((tokens, tokens), 1) < iota((tokens, tokens), 0), 1.0, 0.0)
    rank = jnp.dot(
        after, jnp.where(first_here | second_here, 1.0, 0.0), preferred_element_type=jnp.float32
    )
    first_logit = jnp.zeros((tokens, 1), jnp.float32)
    second_logit = jnp.zeros((tokens, 1), jnp.float32)
    for k in range(ne):
        router_logit = jnp.sum(normed * wide(router_ref[k : k + 1, :]), axis=1, keepdims=True)
        first_logit = first_logit + jnp.where(first_id == k, router_logit, 0.0)
        second_logit = second_logit + jnp.where(second_id == k, router_logit, 0.0)
    first_gate = 1.0 / (1.0 + jnp.exp(second_logit - first_logit))
    second_gate = 1.0 / (1.0 + jnp.exp(first_logit - second_logit))
    gate = jnp.where(first_here, first_gate, jnp.where(second_here, second_gate, 0.0))
    four = jnp.where(rank == wide(line_lane & 3), gate, 0.0)
    fifth = jnp.where(rank == 4.0, gate, 0.0)

    def two_terms(weights):
        weights = jnp.concatenate(weights, axis=0)
        coarse = wide(weights.astype(bf16))
        return jnp.concatenate([coarse, weights - coarse], axis=0).astype(bf16)

    mix_four = two_terms([jnp.where(line_lane < 4, four, 0.0), jnp.where(line_lane < 4, 0.0, four)])
    mix_fifth = two_terms([jnp.where(line_lane == g, fifth, 0.0) for g in range(8)])

    sources = 2 * ne
    moved = (sources * 8, sources * 8)

    def four_place(axis):
        index = iota(moved, axis)
        side = jnp.where(index < sources * 4, 0, 1)
        within = index - side * (sources * 4)
        target = lax.shift_right_logical(within, 2) * 8 + side * 4 + (within & 3)
        return jnp.where(target == iota(moved, 1 - axis), 1.0, 0.0).astype(bf16)

    def fifth_place(axis):
        index, target = iota(moved, axis), iota(moved, 1 - axis)
        fits = ((target & 7) * sources + lax.shift_right_logical(target, 3)) == index
        return jnp.where(fits, 1.0, 0.0).astype(bf16)

    open_four, open_fifth = four_place(0), fifth_place(0)
    close_four, close_fifth = four_place(1), fifth_place(1)

    def plane_push(src_slot, dst_slot, j, partner):
        return push(
            xs.at[src_slot, core, :, :, cols(j)],
            xs.at[dst_slot, core, :, :, cols(j)],
            c_send.at[0],
            c_recv.at[j, dst_slot - 1],
            partner,
        )

    c_copies, m_copies = {}, {}

    def mate_push(slot, j):
        m_copies[j, slot] = push(
            xs.at[slot, core, :, :, cols(j)],
            xs.at[slot, core, :, :, cols(j)],
            m_send.at[0],
            m_recv.at[j],
            mate,
        )
        m_copies[j, slot].start()

    def open_pair(p):
        landed(zin.at[: sources - 1, :, packed(p)], z_send.at[0], z_recv.at[p], mate)
        block_rows = wide(zin[:, :, packed(p)])
        fours = product(
            open_four, block_rows[:, :, :cw].reshape(sources * 8, cw).astype(bf16)
        ).reshape(2, ne, 8, cw)
        fifths = product(
            open_fifth, block_rows[:, :, cw:].reshape(sources * 8, zw - cw).astype(bf16)
        )
        for side in range(2):
            j = 2 * p + side
            xs[0, core, 0:ne, :, cols(j)] = fours[side].astype(bf16)
            row = [
                fifths[g * sources : (g + 1) * sources] for g in range(side * 4, side * 4 + 4)
            ]
            xs[0, core, ne, :, cols(j)] = jnp.concatenate(row, axis=1).astype(bf16)
            for slot, partner in ((1, across), (2, along)):
                c_copies[j, slot] = plane_push(0, slot, j, partner)
                c_copies[j, slot].start()
            mate_push(0, j)

    def relay(j):
        source, partner = (1, along) if j % 2 == 0 else (2, across)
        c_copies[j, source].wait_recv()
        c_copies[j, 3] = plane_push(source, 3, j, partner)
        c_copies[j, 3].start()
        mate_push(source, j)
        c_copies[j, 3 - source].wait_recv()
        mate_push(3 - source, j)

    def corner(j):
        c_copies[j, 3].wait_recv()
        mate_push(3, j)

    tile = min(256, hidden)

    def expand(j):
        landed(xs.at[:, other, :, :, cols(j)], m_send.at[0], m_recv.at[j], mate)
        for h in range(2):
            xl[h] = wide(xs[:, h, :, :, cols(j)]).reshape(rows, cw).astype(bf16)
        pltpu.make_async_copy(
            head_hbm.at[pl.ds(0, 4 * cw), pl.ds(0, hidden)], big.at[pl.ds(0, 4 * cw)], w_sem.at[j]
        ).wait()

        for i in range(hidden // tile):
            where = pl.ds(i * tile, tile)

            def raw(which):
                low = which * width + j * cw
                return product(xl[0], big[low : low + cw, where]) + product(
                    xl[1], big[low + half : low + half + cw, where]
                )

            g, u = raw(0), raw(1)
            if j > 0:
                g, u = g + g_acc[:, where], u + u_acc[:, where]
            if j < n - 1:
                g_acc[:, where] = g
                u_acc[:, where] = u
            else:
                hid[:, where] = (g / (1.0 + jnp.exp(-g)) * u).astype(bf16)

    run(FIRST_ORDER, {"p": open_pair, "r": relay, "c": corner, "e": expand})

    head_loads = []
    per_half = half // block
    for q in range(per_half):
        for h in range(2):
            place = h * per_half + q
            head_loads.append(
                pltpu.make_async_copy(
                    head_hbm.at[:, pl.ds(place * block, block)],
                    big.at[pl.ds(place * share, share)],
                    h_sem.at[place],
                )
            )
            head_loads[-1].start()
    down_load.wait()

    rp, yc, xc, zc, gz, gx = {}, {}, {}, {}, {}, {}

    def down(j):
        def part(side):
            where = pl.ds(pl.multiple_of(side * half + j * cw, 128), cw)
            return product(hid[...], wd[:, where])

        pm[:, :, :, cols(j)] = part(other).reshape(4, tiles, 8, cw).astype(bf16)
        rp[j] = push(
            pm.at[:, :, :, cols(j)], rpair.at[:, :, :, cols(j)], r_send.at[0], r_recv.at[j, 0], mate
        )
        rp[j].start()
        po[:, :, cols(j)] = part(core).reshape(4, chip_rows, cw)

    def pair_sum(j):
        rp[j].wait_recv()
        total = po[:, :, cols(j)] + wide(rpair[:, :, :, cols(j)]).reshape(4, chip_rows, cw)
        kept, passed, partner = ((0, 1), (2, 3), along) if j % 2 == 0 else ((0, 2), (1, 3), across)
        for i in range(2):
            sy[i, :, :, cols(j)] = total[passed[i]].reshape(tiles, 8, cw).astype(bf16)
        yc[j] = push(
            sy.at[:, :, :, cols(j)], ry.at[:, :, :, cols(j)], r_send.at[1], r_recv.at[j, 1], partner
        )
        yc[j].start()
        for i in range(2):
            po[i, :, cols(j)] = total[kept[i]]

    def side_sum(j):
        yc[j].wait_recv()
        total = po[1, :, cols(j)] + wide(ry[1, :, :, cols(j)]).reshape(chip_rows, cw)
        sx[:, :, cols(j)] = total.reshape(tiles, 8, cw).astype(bf16)
        partner = across if j % 2 == 0 else along
        xc[j] = push(
            sx.at[:, :, cols(j)], rx.at[:, :, cols(j)], r_send.at[2], r_recv.at[j, 2], partner
        )
        xc[j].start()
        po[0, :, cols(j)] = po[0, :, cols(j)] + wide(ry[0, :, :, cols(j)]).reshape(chip_rows, cw)

    def own_sum(j):
        xc[j].wait_recv()
        po[0, :, cols(j)] = po[0, :, cols(j)] + wide(rx[:, :, cols(j)]).reshape(chip_rows, cw)
        if j % 2 == 0:
            return
        p = j // 2
        total = po[0, :, p * pw : (p + 1) * pw]
        fours = product(close_four, stacked(total[: sources * 4], 2).astype(bf16))
        fifths = product(close_fifth, stacked(total[sources * 4 :], 8).astype(bf16))
        zs[:, :, :, p * zw : p * zw + cw] = fours.reshape(ne, 2, 8, cw).astype(bf16)
        zs[:, :, :, p * zw + cw : (p + 1) * zw] = fifths.reshape(ne, 2, 8, zw - cw).astype(bf16)
        for slot, to, ct, where in column:
            zc[p, slot] = push(
                zs.at[to, ct, :, packed(p)],
                zo.at[e * 2 + core, :, packed(p)],
                o_send.at[0],
                o_recv.at[p],
                where,
            )
            zc[p, slot].start()
        zo[e * 2 + core, :, packed(p)] = zs[e, core, :, packed(p)]

    squares = [jnp.zeros((tokens, 1), jnp.float32)]

    def mix(p):
        landed(zo.at[: sources - 1, :, packed(p)], o_send.at[0], o_recv.at[p], mate)
        every = wide(zo[:, :, packed(p)]).reshape(ne, 2, 8, zw)
        for h in range(2):
            fours = product(mix_four, every[:, h, :, :cw].reshape(ne * 8, cw).astype(bf16))
            fours = fours[: 2 * tokens] + fours[2 * tokens :]
            fifths = product(mix_fifth, every[:, h, :, cw:].reshape(ne * 8, zw - cw).astype(bf16))
            fifths = fifths[: 8 * tokens] + fifths[8 * tokens :]
            for side in range(2):
                j = 2 * p + side
                first = h * half + j * cw
                row = [fifths[g * tokens : (g + 1) * tokens] for g in range(side * 4, side * 4 + 4)]
                weighted = fours[side * tokens : (side + 1) * tokens] + jnp.concatenate(row, axis=1)
                mixed = wide(resid_ref[:, first : first + cw]) + weighted
                squares[0] = squares[0] + jnp.sum(mixed * mixed, axis=1, keepdims=True)
                ys[me, j, h] = (mixed * final_gain_ref[:, first : first + cw]).astype(bf16)
        for j in (2 * p, 2 * p + 1):
            for k in range(1, ne):
                near_only = j < n - 2 and k != 2
                gz[j, k] = push(
                    ys.at[me, j],
                    ys.at[me, j],
                    y_send.at[2 if near_only else 0],
                    y_recv.at[j, k - 1],
                    (lax.rem(e + k, ne), v, b),
                )
                if near_only:
                    pl.when(e != (ne - 1 if k == 1 else 0))(gz[j, k].start)
                else:
                    gz[j, k].start()
            turn(j, 0)
        if p == PAIRS - 1:
            share_scale()

    def turn(j, k):
        slot = lax.rem(e + ne - k, ne) * nv + v
        gx[j, k] = push(
            ys.at[slot, j], ys.at[slot, j], y_send.at[1], x_recv.at[j], across
        )
        gx[j, k].start()

    def forward(j):
        for k in (1, 3, 2):
            landed(ys.at[me, j], y_send.at[0], y_recv.at[j, k - 1], mate)
            if k == 2 and j < n - 2:
                slot = lax.rem(e + 2, ne) * nv + v
                onward = push(
                    ys.at[slot, j],
                    ys.at[slot, j],
                    y_send.at[2],
                    y_recv.at[j, 2 - 2 * lax.rem(e, 2)],
                    (lax.rem(3 * e + 1, ne), v, b),
                )
                pl.when((e > 0) & (e < ne - 1))(onward.start)
            turn(j, k)

    head_tile = min(256, share)

    def head(j):
        landed(ys.at[:ne, j], y_send.at[1], x_recv.at[j], across)
        if (j * cw) % block == 0:
            for h in range(2):
                head_loads[(j * cw) // block * 2 + h].wait()
        sides = []
        for h in range(2):
            sides.append(wide(ys[:, j, h]).reshape(peers * tokens, cw).astype(bf16))
        left = (j * cw) % block
        low = (j * cw) // block * share

        for i in range(share // head_tile):
            first = i * head_tile
            found = 0.0
            for h in range(2):
                found = found + lax.dot_general(
                    sides[h],
                    big[pl.ds(low + h * per_half * share + first, head_tile), left : left + cw],
                    (((1,), (1,)), ((), ())),
                    preferred_element_type=jnp.float32,
                )
            if j > 0:
                found = found + logits[:, pl.ds(first, head_tile)]
            logits[:, pl.ds(first, head_tile)] = found

    small = []

    def share_scale():
        scale = lax.rsqrt(squares[0] * (1.0 / width) + epsilon)
        scales[me] = jnp.broadcast_to(scale, (tokens, 128))
        for k in range(1, peers):
            small.append(
                push(scales.at[me], scales.at[me], s_send.at[0], s_recv.at[0], at(k))
            )
            small[-1].start()

    run(
        SECOND_ORDER,
        {
            "d": down,
            "s": pair_sum,
            "a": side_sum,
            "b": own_sum,
            "m": mix,
            "f": forward,
            "h": head,
        },
    )

    landed(scales.at[: peers - 1], s_send.at[0], s_recv.at[0], mate)
    group = peers * tokens
    lanes = 128
    scaled = logits[...] * scales[...].reshape(group, lanes)[:, 0:1]
    targets = as_column(wide(target_ref[...]), group)
    vocab_ids = wide(iota((group, share), 1) + me * share)
    top = jnp.max(scaled, axis=1, keepdims=True)
    total = jnp.sum(jnp.exp(scaled - top), axis=1, keepdims=True)
    hit = jnp.sum(jnp.where(vocab_ids == targets, scaled, 0.0), axis=1, keepdims=True)
    line = iota((8, lanes), 0)
    stats[me] = jnp.where(
        line == 0,
        as_row(top, lanes),
        jnp.where(line == 1, as_row(total, lanes), jnp.where(line == 2, as_row(hit, lanes), 0.0)),
    )
    sends = [
        push(stats.at[me], stats.at[me], s_send.at[1], s_recv.at[1], at(k))
        for k in range(1, peers)
    ]
    for copy in sends:
        copy.start()

    choices = length_ref.shape[1]
    lengths_row, questions_row = wide(length_ref[...]), wide(question_ref[...])
    lengths, questions = as_column(lengths_row, choices), as_column(questions_row, choices)
    square = (choices, choices)
    ends = jnp.sum(jnp.where(iota(square, 1) <= iota(square, 0), lengths_row, 0.0), axis=1, keepdims=True)
    place = wide(iota((choices, lanes), 1))
    member = (place >= ends - lengths) & (place < ends)
    same = questions == questions_row

    landed(stats.at[: peers - 1], s_send.at[1], s_recv.at[1], mate)
    every = stats[...]
    best = jnp.max(every[:, 0:1, :], axis=0)
    summed = jnp.sum(every[:, 1:2, :] * jnp.exp(every[:, 0:1, :] - best[None]), axis=0)
    chosen = jnp.sum(every[:, 2:3, :], axis=0)
    used = iota((1, lanes), 1) < group
    logprob = jnp.where(used, chosen - (best + jnp.log(jnp.where(used, summed, 1.0))), 0.0)
    own = jnp.sum(
        jnp.where(iota((tokens, lanes), 1) == iota((tokens, lanes), 0) + me * tokens, logprob, 0.0),
        axis=1,
        keepdims=True,
    )
    found = as_row(own, lanes)
    average = jnp.sum(jnp.where(member, logprob, 0.0), axis=1, keepdims=True) / lengths
    question_top = jnp.max(
        jnp.where(same, as_row(average, choices), -jnp.inf), axis=1, keepdims=True
    )
    raised = jnp.exp(average - question_top)
    denominator = jnp.sum(jnp.where(same, as_row(raised, choices), 0.0), axis=1, keepdims=True)
    prob = raised / denominator
    far = iota((choices, lanes), 1) == iota((choices, lanes), 0) + tokens
    out_ref[...] = found + jnp.sum(jnp.where(far, prob, 0.0), axis=0, keepdims=True)

    for ref, send, recv in (
        (zin.at[: 2 * ne - 1], z_send.at[0], z_recv.at[0]),
        (xs.at[:3, 0], c_send.at[0], c_recv.at[0, 0]),
        (xs.at[:, 0], m_send.at[0], m_recv.at[0]),
        (pm, r_send.at[0], r_recv.at[0, 0]),
        (sy, r_send.at[1], r_recv.at[0, 1]),
        (sx, r_send.at[2], r_recv.at[0, 2]),
        (zo.at[: 2 * ne - 1], o_send.at[0], o_recv.at[0]),
        (ys.at[:2, : n - 1], y_send.at[0], y_recv.at[0, 0]),
        (ys.at[:ne], y_send.at[1], x_recv.at[0]),
        (scales.at[: peers - 1], s_send.at[0], s_recv.at[0]),
        (stats.at[: peers - 1], s_send.at[1], s_recv.at[1]),
    ):
        sent(ref, send, recv, mate)

    @pl.when((e > 0) & (e < ne - 1))
    def _():
        sent(ys.at[:2], y_send.at[2], y_recv.at[0, 0], mate)

    @pl.when((e == 0) | (e == ne - 1))
    def _():
        sent(ys.at[0, : n - 2], y_send.at[2], y_recv.at[0, 0], mate)


def fused_call(sizes, resid, moe_gain, final_gain, router, ids, targets, lengths, questions, *weights):
    ne, nv, nb = sizes
    tokens, width = resid.shape
    w_gate, _, _, lm_head = weights
    hidden = w_gate.shape[2]
    share = lm_head.shape[0]
    cap = row_cap(ne, tokens, ids.shape[0])
    half = width // 2
    tiles = ne * 2 * cap // 8
    rows = 4 * tiles * 8
    peers = ne * nv
    n = CHUNKS
    cw = half // n
    zw = half * 5 // 8
    bf16, f32 = jnp.bfloat16, jnp.float32
    dma = pltpu.SemaphoreType.DMA
    vmem = pltpu.VMEM
    vm = pl.BlockSpec(memory_space=pltpu.VMEM)
    anywhere = pl.BlockSpec(memory_space=pl.ANY)
    return pl.pallas_call(
        functools.partial(fused_kernel, ne, nv, nb, cap),
        out_shape=pltpu.VMEM((1, 128), f32),
        in_specs=[anywhere] * 12,
        out_specs=vm,
        scratch_shapes=[
            vmem(resid.shape, bf16),
            vmem(moe_gain.shape, f32),
            vmem(final_gain.shape, f32),
            vmem(router.shape, bf16),
            vmem(ids.shape, jnp.int32),
            vmem(targets.shape, jnp.int32),
            vmem(lengths.shape, jnp.int32),
            vmem(questions.shape, jnp.int32),
            vmem((2 * width, hidden), bf16),
            vmem((hidden, width), bf16),
            vmem((2, ne, 8, zw), bf16),
            vmem((2 * ne, 8, zw), bf16),
            vmem((4, 2, tiles, 8, half), bf16),
            vmem((2, rows, cw), bf16),
            vmem((rows, hidden), f32),
            vmem((rows, hidden), f32),
            vmem((rows, hidden), bf16),
            vmem((4, tiles, 8, half), bf16),
            vmem((4, tiles * 8, half), f32),
            vmem((4, tiles, 8, half), bf16),
            vmem((2, tiles, 8, half), bf16),
            vmem((2, tiles, 8, half), bf16),
            vmem((tiles, 8, half), bf16),
            vmem((tiles, 8, half), bf16),
            vmem((ne, 2, 8, zw), bf16),
            vmem((2 * ne, 8, zw), bf16),
            vmem((peers, n, 2, 8, cw), bf16),
            vmem((peers * tokens, share), f32),
            vmem((peers, tokens, 128), f32),
            vmem((peers, 8, 128), f32),
            dma((8,)),
            dma((n,)),
            dma((1,)),
            dma((width // hidden,)),
            dma((1,)),
            dma((PAIRS,)),
            dma((1,)),
            dma((n, 3)),
            dma((1,)),
            dma((n,)),
            dma((3,)),
            dma((n, 3)),
            dma((1,)),
            dma((PAIRS,)),
            dma((3,)),
            dma((n, 3)),
            dma((n,)),
            dma((2,)),
            dma((2,)),
        ],
        compiler_params=pltpu.CompilerParams(
            collective_id=0, has_side_effects=True, vmem_limit_bytes=VMEM_BYTES - 1024 * 1024
        ),
        name="fused",
    )(resid, moe_gain, final_gain, router, ids, targets, lengths, questions, *weights)


def kernel_fits(sizes, *arrays):
    ne, nv, nb = sizes
    resid, w_gate, lm_head, ids = arrays[0], arrays[4], arrays[7], arrays[8]
    tokens, width = resid.shape[1:]
    hidden = w_gate.shape[2]
    share = lm_head.shape[0]
    cap = row_cap(ne, tokens, ids.shape[2])
    rows = 8 * ne * cap
    need = 2 * (3 * width * hidden + rows * (4 * width + 6 * hidden) + 8 * ne * 8 * width)
    return (
        ne == 4
        and nv == 2
        and nb == 4
        and tokens == 8
        and ids.shape[2] == 2
        and cap == 5
        and ne * 2 * cap % 8 == 0
        and width % (2 * hidden) == 0
        and width % (2 * CHUNKS * 512) == 0
        and hidden % (width // 2 // CHUNKS) == 0
        and hidden % 256 == 0
        and share == 2 * hidden
        and CHUNKS == 6
        and ne * nv * tokens <= 128
        and need < VMEM_BYTES - 4 * 1024 * 1024
    )


def on_device_kernel(
    sizes,
    resid,
    moe_gain,
    final_gain,
    router,
    w_gate,
    w_up,
    w_down,
    lm_head,
    expert_ids,
    target_ids,
    choice_len,
    choice_question,
):
    found = fused_call(
        sizes,
        resid[0],
        moe_gain.reshape(1, -1),
        final_gain.reshape(1, -1),
        router.T,
        expert_ids[0].T,
        target_ids,
        choice_len,
        choice_question,
        w_gate,
        w_up,
        w_down,
        lm_head,
    )
    tokens = resid.shape[1]
    return found[:, :tokens], found[:, tokens : tokens + choice_len.shape[1]]


def either(sizes, *arrays):
    if kernel_fits(sizes, *arrays):
        return on_device_kernel(sizes, *arrays)
    return on_device(*arrays)


def solution(mesh):
    sizes = tuple(mesh.shape[axis] for axis in ("expert", "vocab", "batch"))
    return jax.shard_map(
        functools.partial(either, sizes),
        mesh=mesh,
        in_specs=(
            P("batch", ("expert", "vocab"), None),
            P(),
            P(),
            P(),
            P("expert", None, ("vocab", "batch")),
            P("expert", None, ("vocab", "batch")),
            P("expert", ("vocab", "batch"), None),
            P(("expert", "vocab"), None),
            P("batch", ("expert", "vocab"), None),
            P("batch", None),
            P("batch", None),
            P("batch", None),
        ),
        out_specs=(P("batch", ("expert", "vocab")), P("batch", None)),
        check_vma=False,
    )
```
